32 devices in a mesh: gx: 8 (over z, y), gy: 4 (over x, core).
Axes of the slice: x: 2, y: 2, z: 4, core: 2. Of those that a mesh axis runs over, the one named last changes fastest.
Arguments:
- disp_now: float32 [3, 8, 128, 512], P(None, None, 'gx', 'gy'), may hold values from -6 to 6
- disp_prev: float32 [3, 8, 128, 512], P(None, None, 'gx', 'gy'), may hold values from -6 to 6
- density: float32 [8, 128, 512], P(None, 'gx', 'gy'), may hold values from 1 to 2
- moduli: float32 [2, 8, 128, 512], P(None, None, 'gx', 'gy'), may hold values from 0.3 to 1
- coarse: float32 [64, 24, 256], P(('gx', 'gy')), may hold values from -6 to 6
- block_route: int32 [64], replicated, may hold values from 0 to 127, as said below
- ranges: int32 [8, 4, 2], P('gx', 'gy'), may hold values from 1 to 8, as said below
- offsets: int32 [8, 4, 4, 3], P('gx', 'gy'), may hold values from 0 to 24, as said below
Outputs:
- incident: float32 [2, 3, 8, 128, 512], P(None, None, None, 'gx', 'gy')
- disp_mid: float32 [3, 8, 128, 512], P(None, None, 'gx', 'gy')
- disp_next: float32 [3, 8, 128, 512], P(None, None, 'gx', 'gy')
The draws below stay inside these ranges and needn't reach their ends.
Inputs may be any that keep to these rules, and one draw needn't show every extreme that they name: block_route[b] = tile 4 + g with tile = X 4 + Y; no slot is named twice; the slots named of a tile are g = 0 to k - 1 for its count k, which is 1 on half of the tiles, 2 on a quarter and 4 on a quarter. ranges[X, Y] = (lo, hi) with hi = 2 k for the tile's count k in block_route, and 1 <= lo < hi. offsets[X, Y, g] = (oz, oe, on) in fine cells with oz at most 5.
All inputs are finite; a program needn't handle non-finite values.
Results may differ from the reference program's by a relative error of at most 0.000073.
Values sent between devices are 32-bit elements; how exact they have to be, the bound alone decides.
No kernel may reach another device: no remote copies, remote signals or barrier semaphores. Data moves between devices by JAX's collectives and lax.ppermute only.
A program may use at most 64 MiB of HBM per device.

```python
import math
import jax
import jax.numpy as jnp
from jax import lax

LEV = 8
CE = 16
CN = 128
NT = 4
G = 4
CEC = 8
CNC = 26
PTS = 256
TILES = 32
BLOCKS = 64
NE = 128
NN = 512
N_GX = 8
N_GY = 4


def plan_tiles(key):
    tile_perm = jax.random.permutation(jax.random.fold_in(key, 101), TILES)
    tile_rank = jnp.argsort(tile_perm).astype(jnp.int32)
    quarter = TILES // 4
    counts = jnp.where(tile_rank < quarter, G, jnp.where(tile_rank < 2 * quarter, 2, 1)).astype(jnp.int32)
    slot_ids = jnp.arange(TILES * G, dtype=jnp.int32)
    slot_tile = slot_ids // G
    slot_group = slot_ids % G
    unused = (slot_group >= counts[slot_tile]).astype(jnp.int32)
    slot_key = unused * (TILES * G) + tile_rank[slot_tile] * G + slot_group
    ordered = jnp.argsort(slot_key)[:BLOCKS].astype(jnp.int32)
    spread_perm = jax.random.permutation(jax.random.fold_in(key, 102), BLOCKS).astype(jnp.int32)
    position = jnp.arange(BLOCKS, dtype=jnp.int32)
    place_key = 4 + spread_perm
    place_key = jnp.where(position == 0, 0, place_key)
    place_key = jnp.where(position == 1, 1, place_key)
    place_key = jnp.where(position == 2 * N_GY, 2, place_key)
    place_key = jnp.where(position == 2 * N_GY + 1, 3, place_key)
    place_rank = jnp.argsort(jnp.argsort(place_key)).astype(jnp.int32)
    routing = ordered[place_rank]
    high_level = 2 * counts
    low_level = jax.random.randint(jax.random.fold_in(key, 103), (TILES,), 1, high_level)
    ranges = jnp.stack([low_level, high_level], axis=-1).reshape(N_GX, N_GY, 2)
    return (routing.astype(jnp.int32), ranges.astype(jnp.int32))


def draw_block_route(key, part):
    return plan_tiles(key)[0]


def draw_ranges(key, part):
    return plan_tiles(key)[1]


def draw_offsets(key, part):
    level_part = jax.random.randint(jax.random.fold_in(key, 201), (N_GX, N_GY, G, 1), 0, 6)
    east_part = jax.random.randint(jax.random.fold_in(key, 202), (N_GX, N_GY, G, 1), 0, 25)
    north_part = jax.random.randint(jax.random.fold_in(key, 203), (N_GX, N_GY, G, 1), 0, 25)
    return jnp.concatenate([level_part, east_part, north_part], axis=-1).astype(jnp.int32)


def block_levels(own_key, shape, shards, least, largest):
    loudness = 1.0
    for dim, shards_of in shards:
        draws = jax.random.uniform(jax.random.fold_in(jax.random.fold_in(own_key, 6), dim), (shards_of,), jnp.float32, least / len(shards), largest / len(shards))
        loudness = loudness * jnp.repeat(jnp.exp(draws), shape[dim] // shards_of).reshape((-1,) + (1,) * (len(shape) - 1 - dim))
    return loudness


def normal_values(own_key, extent, scale, limit, split=(), kind=jnp.bfloat16):
    drawn = jax.random.normal(own_key, extent, jnp.float32) * scale
    if len(split) > 0:
        drawn = block_levels(own_key, extent, split, -0.22, 0.18) * drawn
    return jnp.clip(drawn, min=-limit, max=limit).astype(kind)


def setup_inputs(seed: int = 0) -> dict:
    splits = jax.random.split(jax.random.key(seed), 9)
    return {
        "disp_now": normal_values(splits[0], (3, LEV, NE, NN), 1.0, 6.0, ((2, 8), (3, 4)), jnp.float32),
        "disp_prev": normal_values(splits[1], (3, LEV, NE, NN), 1.0, 6.0, ((2, 8), (3, 4)), jnp.float32),
        "density": jnp.clip(jnp.exp(math.log(2.0) - 0.6931472 * jax.random.uniform(splits[2], (LEV, NE, NN), jnp.float32) ** block_levels(splits[2], (LEV, NE, NN), ((1, 8), (2, 4)), -0.2, 0.2)), 1.0, 2.0),
        "moduli": jnp.clip(jnp.exp(math.log(1.0) - 1.2039728 * jax.random.uniform(splits[3], (2, LEV, NE, NN), jnp.float32) ** block_levels(splits[3], (2, LEV, NE, NN), ((2, 8), (3, 4)), -0.2, 0.2)), 0.3, 1.0),
        "coarse": normal_values(splits[4], (BLOCKS, NT * 6, PTS), 1.0, 6.0, ((0, 32),), jnp.float32),
        "block_route": draw_block_route(jax.random.fold_in(splits[8], 71), 0),
        "ranges": draw_ranges(jax.random.fold_in(splits[8], 71), 0),
        "offsets": draw_offsets(jax.random.fold_in(splits[8], 71), 0),
    }


step_square = 0.05
time_weights = ((-0.0595, 0.7735, 0.3315, -0.0455), (-0.063756, 0.607068, 0.517132, -0.060444))


def trimmed(values_in, axis_pos, head_cut, tail_cut):
    axis_pos = axis_pos % values_in.ndim
    return lax.slice_in_dim(values_in, head_cut, values_in.shape[axis_pos] - tail_cut, axis=axis_pos)


def inner_cut(values_in, axes_list):
    for axis_pos in axes_list:
        values_in = trimmed(values_in, axis_pos, 1, 1)
    return values_in


def operate(motion, shear_mod, lame_mod):
    spatial = (-3, -2, -1)
    stiffness = lame_mod + 2.0 * shear_mod
    components = []
    for i in range(3):
        component = motion[..., i, :, :, :]
        total = None
        for j in range(3):
            axis_along = spatial[j]
            others = tuple(a for a in spatial if a != axis_along)
            modulus = stiffness if j == i else shear_mod
            values = inner_cut(component, others)
            weights = inner_cut(modulus, others)
            middle = trimmed(values, axis_along, 1, 1)
            forward = trimmed(values, axis_along, 2, 0)
            backward = trimmed(values, axis_along, 0, 2)
            modulus_mid = trimmed(weights, axis_along, 1, 1)
            modulus_next = trimmed(weights, axis_along, 2, 0)
            modulus_prior = trimmed(weights, axis_along, 0, 2)
            flux_term = 0.5 * (modulus_mid + modulus_next) * (forward - middle) - 0.5 * (modulus_mid + modulus_prior) * (middle - backward)
            total = flux_term if total is None else total + flux_term
        for j in range(3):
            if j != i:
                across = spatial[i]
                axis_along = spatial[j]
                third_axis = [a for a in spatial if a != across and a != axis_along][0]
                partner = motion[..., j, :, :, :]
                gradient = 0.5 * (trimmed(partner, axis_along, 2, 0) - trimmed(partner, axis_along, 0, 2))
                flux_term = trimmed(lame_mod, axis_along, 1, 1) * gradient
                total = total + trimmed(0.5 * (trimmed(flux_term, across, 2, 0) - trimmed(flux_term, across, 0, 2)), third_axis, 1, 1)
                gradient = 0.5 * (trimmed(partner, across, 2, 0) - trimmed(partner, across, 0, 2))
                flux_term = trimmed(shear_mod, across, 1, 1) * gradient
                total = total + trimmed(0.5 * (trimmed(flux_term, axis_along, 2, 0) - trimmed(flux_term, axis_along, 0, 2)), third_axis, 1, 1)
        components.append(total)
    return jnp.stack(components, axis=-4)


def hat_matrix(offset_cells, fine_count, coarse_count):
    fine_pos = (offset_cells[:, None] + jnp.arange(fine_count, dtype=jnp.int32)[None, :]) * 4
    base_index = fine_pos // 25
    fraction = (fine_pos % 25).astype(jnp.float32) / 25.0
    column = jnp.arange(coarse_count, dtype=jnp.int32)
    first = jnp.where(column[None, None, :] == base_index[:, :, None], 1.0 - fraction[:, :, None], 0.0)
    second = jnp.where(column[None, None, :] == base_index[:, :, None] + 1, fraction[:, :, None], 0.0)
    return first + second


def spread(samples, offset_cells, east_cells, north_cells):
    level_pos = (offset_cells[:, 0:1] + jnp.arange(2, dtype=jnp.int32)[None, :]).astype(jnp.float32) * (4.0 / 25.0)
    upper_level = samples[:, :, :, 0][:, :, :, None]
    lower_level = samples[:, :, :, 1][:, :, :, None]
    vertical = upper_level * (1.0 - level_pos)[:, None, None, :, None, None] + lower_level * level_pos[:, None, None, :, None, None]
    east_matrix = hat_matrix(offset_cells[:, 1], east_cells, samples.shape[-2])
    north_matrix = hat_matrix(offset_cells[:, 2], north_cells, samples.shape[-1])
    eastern = jnp.einsum("kxa,kncjay->kncjxy", east_matrix, vertical, precision=lax.Precision.HIGHEST)
    return jnp.einsum("kncjxa,kya->kncjxy", eastern, north_matrix, precision=lax.Precision.HIGHEST)


def pad_cells(values_in):
    return jnp.pad(values_in, [(0, 0)] * (values_in.ndim - 3) + [(1, 1), (1, 1), (1, 1)])


def reference(disp_now, disp_prev, density, moduli, coarse, block_route, ranges, offsets):
    weights = jnp.array(time_weights, jnp.float32)
    used = coarse[:, :, :CEC * CNC]
    timed_blocks = jnp.einsum("nt,ktpq->knpq", weights, used.reshape(BLOCKS, NT, 6, CEC * CNC), precision=lax.Precision.HIGHEST)
    samples = timed_blocks.reshape(BLOCKS, 2, 3, 2, CEC, CNC)
    shifts = offsets.reshape(TILES * G, 3)[block_route]
    fine_values = spread(samples, shifts, CE, CN)
    placed = jnp.zeros((TILES * G, 2, 3, 2, CE, CN), jnp.float32).at[block_route].set(fine_values)
    incident = placed.reshape(N_GX, N_GY, G, 2, 3, 2, CE, CN).transpose(3, 4, 2, 5, 0, 6, 1, 7).reshape(2, 3, LEV, N_GX * CE, N_GY * CN)
    low_full = jnp.repeat(jnp.repeat(ranges[:, :, 0], CE, axis=0), CN, axis=1)
    high_full = jnp.repeat(jnp.repeat(ranges[:, :, 1], CE, axis=0), CN, axis=1)
    level_ids = jnp.arange(LEV, dtype=jnp.int32)[:, None, None]
    outer_mask = (level_ids < low_full[None]).astype(jnp.float32)
    inner_mask = ((level_ids >= low_full[None]) & (level_ids < high_full[None])).astype(jnp.float32)
    shear_pad = pad_cells(moduli[0])
    lame_pad = pad_cells(moduli[1])

    def applied(values_in):
        return operate(pad_cells(values_in), shear_pad, lame_pad)

    force_first = inner_mask * applied(outer_mask * incident[0]) - outer_mask * applied(inner_mask * incident[0])
    force_second = inner_mask * applied(outer_mask * incident[1]) - outer_mask * applied(inner_mask * incident[1])

    def advance(current, previous, forcing):
        return 2.0 * current - previous + step_square / density * (applied(current) + forcing)

    disp_mid = advance(disp_now, disp_prev, force_first)
    disp_next = advance(disp_mid, disp_now, force_second)
    return incident, disp_mid, disp_next
```

```python
import functools

import jax
import jax.numpy as jnp
from jax import lax
from jax.experimental import pallas as pl
from jax.experimental.pallas import tpu as pltpu
from jax.sharding import PartitionSpec as P

step_square = 0.05
time_weights = ((-0.0595, 0.7735, 0.3315, -0.0455), (-0.063756, 0.607068, 0.517132, -0.060444))

LANE = 128
WIDE = 256
VMEM = pltpu.VMEM
SMEM = pltpu.SMEM


def lane_ids(shape):
    return lax.broadcasted_iota(jnp.int32, shape, len(shape) - 1)


def sub_ids(shape):
    return lax.broadcasted_iota(jnp.int32, shape, len(shape) - 2)


def shift_up(u):
    count = u.shape[0]
    return jnp.where(sub_ids(u.shape) == count - 1, 0.0, pltpu.roll(u, count - 1, 0))


def shift_down(u):
    return jnp.where(sub_ids(u.shape) == 0, 0.0, pltpu.roll(u, 1, 0))


def shift_next(u):
    return pltpu.roll(u, u.shape[1] - 1, 1)


def shift_prior(u):
    return pltpu.roll(u, 1, 1)


def level_row(ref, plane, levels, rows, r):
    return ref[pl.ds(plane * levels * rows + r, levels, stride=rows), :]


def meta_vector(off_ref, rng_ref, groups):
    shape = (8, LANE)
    lane = lane_ids(shape)
    out = jnp.zeros(shape, jnp.float32)
    for g in range(groups):
        for q in range(3):
            out = jnp.where(lane == 3 * g + q, off_ref[0, 0, g, q].astype(jnp.float32), out)
    for q in range(2):
        out = jnp.where(lane == 3 * groups + q, rng_ref[0, 0, q].astype(jnp.float32), out)
    return out


def pre_kernel(
    lev, rows, groups, samples, coarse_ref, now_ref, prev_ref, dens_ref, mod_ref, off_ref, rng_ref,
    pay_ref, first_ref, last_ref, scr
):
    for k in range(coarse_ref.shape[0]):
        mixed = []
        for n in range(2):
            total = None
            for t in range(samples):
                term = time_weights[n][t] * coarse_ref[k, 6 * t : 6 * t + 6, :]
                total = term if total is None else total + term
            mixed.append(total)
        scr[8 * k : 8 * k + 6, :] = mixed[0]
        scr[8 * k + 6 : 8 * k + 8, :] = mixed[1][0:2]
        scr[16 + 4 * k : 20 + 4 * k, :] = mixed[1][2:6]
    head = [scr[8 * i : 8 * i + 8, :LANE] for i in range(3)]
    tail = [scr[8 * i : 8 * i + 8, LANE:] for i in range(3)]
    lane = lane_ids((8, LANE))
    tiles = head + [
        jnp.where(lane < 80, tail[0], pltpu.roll(tail[2], 80, 1)),
        jnp.where(lane < 80, tail[1], pltpu.roll(tail[2], 40, 1)),
    ]

    def send(d, carry):
        for i, tile in enumerate(tiles):
            pay_ref[d, 8 * i : 8 * i + 8, :] = tile
        return carry

    lax.fori_loop(0, pay_ref.shape[0], send, 0)
    meta = meta_vector(off_ref, rng_ref, groups)
    for ref, start, edge in ((first_ref, 0, 0), (last_ref, rows - 2, rows - 1)):
        for c in range(3):
            for r in range(2):
                ref[2 * c + r] = level_row(now_ref, c, lev, rows, start + r)
            ref[10 + c] = level_row(prev_ref, c, lev, rows, edge)
        for k in range(2):
            for r in range(2):
                ref[6 + 2 * k + r] = level_row(mod_ref, k, lev, rows, start + r)
        ref[13] = level_row(dens_ref, 0, lev, rows, edge)
        ref[14] = meta


def plane_row(refs, lev, rows, plane, x):
    now_ref, prev_ref, dens_ref, mod_ref, before_ref, after_ref = refs
    if plane < 3:
        source, own, strip, both = now_ref, plane, 2 * plane, True
    elif plane < 5:
        source, own, strip, both = mod_ref, plane - 3, 6 + 2 * (plane - 3), True
    elif plane < 8:
        source, own, strip, both = prev_ref, plane - 5, 10 + plane - 5, False
    else:
        source, own, strip, both = dens_ref, 0, 13, False
    if 2 <= x < rows + 2:
        return level_row(source, own, lev, rows, x - 2)
    ref, r = (before_ref, x) if x < 2 else (after_ref, x - rows - 2)
    if both:
        return ref[strip + r]
    return ref[strip] if x in (1, rows + 2) else None


def pack_kernel(
    lev, rows, groups, now_ref, prev_ref, dens_ref, mod_ref, before_ref, after_ref, off_ref, rng_ref,
    west_ref, east_ref, meta_ref
):
    refs = (now_ref, prev_ref, dens_ref, mod_ref, before_ref, after_ref)
    lane = lane_ids((lev, LANE))
    span = 2 * (rows + 4)
    for block in range(3):
        west = jnp.zeros((lev, LANE), jnp.float32)
        east = jnp.zeros((lev, LANE), jnp.float32)
        for p in range(3):
            for x in range(rows + 4):
                v = plane_row(refs, lev, rows, 3 * block + p, x)
                if v is None:
                    continue
                at = span * p + 2 * x
                here = (lane == at) | (lane == at + 1)
                west = jnp.where(here, pltpu.roll(v, at, 1), west)
                east = jnp.where(here, pltpu.roll(v, (at + 2) % LANE, 1), east)
        west_ref[block] = west
        east_ref[block] = east
    sub = sub_ids((lev, LANE))
    meta = meta_vector(off_ref, rng_ref, groups)
    both = jnp.where(sub == 0, before_ref[14], jnp.where(sub == 1, meta, after_ref[14]))
    west_ref[3] = both
    east_ref[3] = both
    meta_ref[...] = both


MU = {"l+": 0, "l-": 1, "e+": 2, "e-": 3, "n+": 4, "n-": 5}
STIFF = {"l+": 6, "l-": 7, "e+": 8, "e-": 9, "n+": 10, "n-": 11}
CENTER = 12
MU_QUARTER = 15
LAME_QUARTER = 16
COEFS = 17


def quarter_row(mod_ref, coef_ref, x):
    coef_ref[MU_QUARTER, x] = 0.25 * mod_ref[0, x]
    coef_ref[LAME_QUARTER, x] = 0.25 * mod_ref[1, x]


def coef_row(mod_ref, coef_ref, x):
    sums = []
    for stiff, table in ((False, MU), (True, STIFF)):

        def half(r):
            mu = mod_ref[0, r]
            return 0.5 * mod_ref[1, r] + mu if stiff else 0.5 * mu

        k = half(x)
        values = {
            "l+": k + shift_up(k),
            "l-": k + shift_down(k),
            "e+": k + half(x + 1),
            "e-": k + half(x - 1),
            "n+": k + shift_next(k),
            "n-": k + shift_prior(k),
        }
        for name, value in values.items():
            coef_ref[table[name], x] = value
        sums.append({d: values[d + "+"] + values[d + "-"] for d in "len"})
    soft, hard = sums
    coef_ref[CENTER + 0, x] = hard["l"] + soft["e"] + soft["n"]
    coef_ref[CENTER + 1, x] = soft["l"] + hard["e"] + soft["n"]
    coef_ref[CENTER + 2, x] = soft["l"] + soft["e"] + hard["n"]


def east_flow(u, coef_ref, x):
    mu = coef_ref[MU_QUARTER, x]
    lame = coef_ref[LAME_QUARTER, x]
    rise = [shift_up(u[c]) - shift_down(u[c]) for c in range(2)]
    run = [shift_next(u[c]) - shift_prior(u[c]) for c in (1, 2)]
    return mu * rise[1], lame * (rise[0] + run[1]), mu * run[0]


def apply_row(field, flow, coef_ref, x, width):
    def cut(v):
        return v[:, :width]

    u = [field(c, x) for c in range(3)]
    after = [field(c, x + 1) for c in range(3)]
    before = [field(c, x - 1) for c in range(3)]
    up = [shift_up(v) for v in u]
    down = [shift_down(v) for v in u]
    nxt = [shift_next(v) for v in u]
    prior = [shift_prior(v) for v in u]
    d_l = [up[c] - down[c] for c in range(3)]
    d_n = [nxt[c] - prior[c] for c in range(3)]
    d_e = [after[c] - before[c] for c in range(3)]
    mu = coef_ref[MU_QUARTER, x]
    lame = coef_ref[LAME_QUARTER, x]
    level_flow = (cut(lame * (d_e[1] + d_n[2])), cut(mu * d_e[0]), cut(mu * d_n[0]))
    north_flow = (mu * d_l[2], mu * d_e[2], lame * (d_l[0] + d_e[1]))
    out = []
    for i in range(3):

        def coef(name):
            table = STIFF if "len".index(name[0]) == i else MU
            return cut(coef_ref[table[name], x])

        total = cut(flow(i, x + 1)) - cut(flow(i, x - 1))
        total += shift_up(level_flow[i]) - shift_down(level_flow[i])
        total += cut(shift_next(north_flow[i]) - shift_prior(north_flow[i]))
        total += coef("l+") * cut(up[i]) + coef("l-") * cut(down[i])
        total += coef("e+") * cut(after[i]) + coef("e-") * cut(before[i])
        total += coef("n+") * cut(nxt[i]) + coef("n-") * cut(prior[i])
        total -= cut(coef_ref[CENTER + i, x]) * cut(u[i])
        out.append(total)
    return out


def prep_kernel(
    lev, rows, groups, c_north, now_ref, prev_ref, dens_ref, mod_ref, before_ref, after_ref, west_ref, east_ref, meta_ref,
    route_ref, place_ref, mods_ref, base_ref, scale_ref, mask_ref, level_ref, shift_ref, own_hat_ref, side_hat_ref,
    index_ref, now_x, flow, coef
):
    refs = (now_ref, prev_ref, dens_ref, mod_ref, before_ref, after_ref)
    lane = lane_ids((lev, LANE))
    sub = sub_ids((lev, LANE))
    span = 2 * (rows + 4)
    metas = (meta_ref[...], east_ref[3], west_ref[3])

    for i in range(9 * groups):
        index_ref[i] = 0
    my_x, my_y = place_ref[0], place_ref[1]
    n_y = place_ref[2]

    def find(b, carry):
        slot = route_ref[b]
        tile = lax.div(slot, groups)
        g = slot - tile * groups
        tile_x = lax.div(tile, n_y)
        d_x = tile_x - my_x + 1
        d_y = tile - tile_x * n_y - my_y
        column = jnp.where(d_y < 0, 2, d_y)

        @pl.when((d_x >= 0) & (d_x < 3) & (d_y >= -1) & (d_y < 2))
        def _():
            index_ref[(d_x * 3 + column) * groups + g] = b

        return carry

    lax.fori_loop(0, route_ref.shape[0], find, 0)

    def sides(plane, x):
        block, p = divmod(plane, 3)
        at = span * p + 2 * x
        return jnp.where(
            lane < 2,
            pltpu.roll(east_ref[block], (-at) % LANE, 1),
            jnp.where(lane >= LANE - 2, pltpu.roll(west_ref[block], (LANE - 2 - at) % LANE, 1), 0.0),
        )

    for x in range(rows + 4):
        for c in range(3):
            now_x[c, x, :, :LANE] = plane_row(refs, lev, rows, c, x)
            now_x[c, x, :, LANE:] = sides(c, x)
        for k in range(2):
            mods_ref[k, x, :, :LANE] = plane_row(refs, lev, rows, 3 + k, x)
            mods_ref[k, x, :, LANE:] = sides(3 + k, x)
        if 1 <= x < rows + 3:
            for c in range(3):
                base_ref[c, x, :, :LANE] = plane_row(refs, lev, rows, 5 + c, x)
                base_ref[c, x, :, LANE:] = sides(5 + c, x)
            for part, v in ((slice(0, LANE), plane_row(refs, lev, rows, 8, x)), (slice(LANE, WIDE), sides(8, x))):
                there = v > 0.0
                scale_ref[x, :, part] = jnp.where(there, step_square / jnp.where(there, v, 1.0), 0.0)

    def first(x, carry):
        quarter_row(mods_ref, coef, x)
        parts = east_flow([now_x[c, x] for c in range(3)], coef, x)
        for i in range(3):
            flow[i, x] = parts[i]
        return carry

    lax.fori_loop(0, rows + 4, first, 0)

    def second(x, carry):
        coef_row(mods_ref, coef, x)
        applied = apply_row(lambda c, r: now_x[c, r], lambda i, r: flow[i, r], coef, x, WIDE)
        for c in range(3):
            base_ref[c, x] = 2.0 * now_x[c, x] - base_ref[c, x] + scale_ref[x] * applied[c]
        return carry

    lax.fori_loop(1, rows + 3, second, 0)

    group_of_sub = sub // 2
    second_level = (sub - 2 * group_of_sub).astype(jnp.float32)
    k_row = sub_ids((LANE, LANE))
    k_lane = lane_ids((LANE, LANE))
    sub_f = sub.astype(jnp.float32)
    for t in range(3):
        def entry(column, i):
            return metas[column][t : t + 1, i : i + 1]

        for column in range(3):
            low = entry(column, 3 * groups)
            high = entry(column, 3 * groups + 1)
            outer = (sub_f < low).astype(jnp.float32)
            inner = ((sub_f >= low) & (sub_f < high)).astype(jnp.float32)
            if column == 0:
                mask_ref[0, t, :, :LANE] = outer
                mask_ref[1, t, :, :LANE] = inner
            elif column == 1:
                east_masks = (outer, inner)
            else:
                for q, own in enumerate((outer, inner)):
                    mask_ref[q, t, :, LANE:] = jnp.where(lane < LANE // 2, east_masks[q], own)
            depth = second_level
            east_at = jnp.zeros((lev, LANE), jnp.float32)
            hold = jnp.zeros((lev, LANE), jnp.float32)
            north_at = jnp.zeros((LANE, LANE), jnp.float32)
            point = jnp.zeros((LANE, LANE), jnp.float32)
            for g in range(groups):
                here = group_of_sub == g
                depth = jnp.where(here, second_level + entry(column, 3 * g), depth)
                east_at = jnp.where(here, 4.0 * entry(column, 3 * g + 1), east_at)
                mine = here & (lane >= g * c_north) & (lane < (g + 1) * c_north)
                hold = jnp.where(mine & (high > 2.0 * g + 1.0), 1.0 / 625.0, hold)
                there = (k_row >= g * c_north) & (k_row < (g + 1) * c_north)
                north_at = jnp.where(there, 4.0 * entry(column, 3 * g + 2), north_at)
                point = jnp.where(there, 25.0 * (k_row - g * c_north).astype(jnp.float32), point)
            depth = depth * (4.0 / 25.0)
            level_ref[t, column, 0] = hold * (1.0 - depth)
            level_ref[t, column, 1] = hold * depth
            hat = jnp.maximum(25.0 - jnp.abs(north_at + 4.0 * k_lane.astype(jnp.float32) - point), 0.0)
            hat = jnp.where(k_row < groups * c_north, hat, 0.0)
            if column == 0:
                shift_ref[t, :, :LANE] = east_at
                own_hat_ref[t] = hat.astype(jnp.bfloat16)
            elif column == 1:
                east_shift = east_at
                side_hat_ref[t, :LANE, :] = jnp.where(k_lane < LANE // 2, hat, 0.0).astype(jnp.bfloat16)
            else:
                shift_ref[t, :, LANE:] = jnp.where(lane < LANE // 2, east_shift, east_at)
                side_hat_ref[t, LANE:, :] = jnp.where(k_lane >= LANE // 2, hat, 0.0).astype(jnp.bfloat16)


def split_dot(ref, hat):
    v = ref[...]
    high = v.astype(jnp.bfloat16)
    low = (v - high.astype(jnp.float32)).astype(jnp.bfloat16)
    return jnp.dot(high, hat, preferred_element_type=jnp.float32) + jnp.dot(
        low, hat, preferred_element_type=jnp.float32
    )


def finish_kernel(
    lev, rows, groups, c_east, c_north, block_hold, got_ref, index_ref, mods_ref, base_ref, scale_ref, mask_ref,
    level_ref, shift_ref, own_hat_ref, side_hat_ref, now_ref, inc_out, mid_out, next_out,
    mixed, own_rows, side_rows, north, parts, flow, mid, coef
):
    lane = lane_ids((8, LANE))

    def quarter(x, carry):
        quarter_row(mods_ref, coef, x)
        return carry

    lax.fori_loop(0, rows + 4, quarter, 0)

    def coefs(x, carry):
        coef_row(mods_ref, coef, x)
        return carry

    lax.fori_loop(1, rows + 3, coefs, 0)

    def tile_row(t, carry):
        for column in range(3):
            pieces = []
            for g in range(groups):
                b = index_ref[(t * 3 + column) * groups + g]
                source = lax.div(b, block_hold)
                k = b - source * block_hold
                top = pl.multiple_of(8 * k, 8)
                third = got_ref[source, 24:32, :]
                fourth = got_ref[source, 32:40, :]
                tail = jnp.where(lane < 40, pltpu.roll(third, LANE - 80, 1), pltpu.roll(fourth, LANE - 40, 1))
                pieces.append(
                    (
                        (got_ref[source, pl.ds(top, 8), :], got_ref[source, pl.ds(24 + top, 8), :]),
                        (pltpu.roll(got_ref[source, 16:24, :], 4 * k, 0), pltpu.roll(tail, 4 * k, 0)),
                    )
                )
            for a in range(c_east):
                start = a * c_north
                for half in range(2):
                    total = jnp.zeros((8, LANE), jnp.float32)
                    for g in range(groups):
                        body, tail = pieces[g][half]
                        at = g * c_north
                        if start + c_north <= LANE:
                            moved = pltpu.roll(body, (at - start) % LANE, 1)
                        elif start >= LANE:
                            moved = pltpu.roll(tail, (at - start) % LANE, 1)
                        else:
                            moved = jnp.where(
                                lane < at + LANE - start,
                                pltpu.roll(body, (at - start) % LANE, 1),
                                pltpu.roll(tail, (at - start) % LANE, 1),
                            )
                        total = jnp.where((lane >= at) & (lane < at + c_north), moved, total)
                    mixed[a, 8 * half : 8 * half + 8, :] = total
            w0 = level_ref[t, column, 0]
            w1 = level_ref[t, column, 1]
            for nc in range(6):
                r = (nc // 3) * 6 + 2 * (nc % 3)
                for a in range(c_east):
                    value = w0 * jnp.broadcast_to(mixed[a, r : r + 1, :], (lev, LANE)) + w1 * jnp.broadcast_to(
                        mixed[a, r + 1 : r + 2, :], (lev, LANE)
                    )
                    at = (nc * c_east + a) * lev
                    if column == 0:
                        own_rows[at : at + lev, :] = value
                    elif column == 1:
                        side_rows[at : at + lev, :LANE] = value
                    else:
                        side_rows[at : at + lev, LANE:] = value
        own = split_dot(own_rows, own_hat_ref[t])
        north[t, :, :, :LANE] = own.reshape(6 * c_east, lev, LANE)
        side = split_dot(side_rows, side_hat_ref[t])
        north[t, :, :, LANE:] = side.reshape(6 * c_east, lev, LANE)
        return carry

    lax.fori_loop(0, 3, tile_row, 0)

    near = (4 * 24) // 25 + 3

    def east(x, carry):
        t = (x >= 2).astype(jnp.int32) + (x >= rows + 2).astype(jnp.int32)
        cell = x - 2 + rows - t * rows
        first = lax.div(4 * cell, 25)
        at = shift_ref[t] + (4 * cell - 25 * first).astype(jnp.float32)
        weights = [jnp.maximum(25.0 - jnp.abs(at - 25.0 * i), 0.0) for i in range(near)]
        outer = mask_ref[0, t]
        inner = mask_ref[1, t]
        values = []
        for nc in range(6):
            total = None
            for i in range(near):
                term = weights[i] * north[t, nc * c_east + first + i]
                total = term if total is None else total + term
            values.append(total)
            parts[nc, x] = outer * total
            parts[6 + nc, x] = inner * total

        @pl.when(t == 1)
        def _():
            for nc in range(6):
                inc_out[pl.ds(nc * lev * rows + cell, lev, stride=rows), :] = values[nc][:, :LANE]

        for q, mask in enumerate((outer, inner)):
            moved = east_flow([mask * values[c] for c in range(3)], coef, x)
            for i in range(3):
                flow[3 * q + i, x] = moved[i]
        return carry

    lax.fori_loop(0, rows + 4, east, 0)

    def forcing(step, x, t, width):
        outside = apply_row(
            lambda c, r: parts[3 * step + c, r], lambda i, r: flow[i, r], coef, x, width
        )
        inside = apply_row(
            lambda c, r: parts[6 + 3 * step + c, r], lambda i, r: flow[3 + i, r], coef, x, width
        )
        outer = mask_ref[0, t][:, :width]
        inner = mask_ref[1, t][:, :width]
        return [inner * outside[c] - outer * inside[c] for c in range(3)]

    def middle(x, carry):
        t = (x >= 2).astype(jnp.int32) + (x >= rows + 2).astype(jnp.int32)
        force = forcing(0, x, t, WIDE)
        for c in range(3):
            mid[c, x] = base_ref[c, x] + scale_ref[x] * force[c]
        return carry

    lax.fori_loop(1, rows + 3, middle, 0)

    def flows(x, carry):
        for q, load in enumerate(
            (lambda c: parts[3 + c, x], lambda c: parts[9 + c, x], lambda c: mid[c, x])
        ):
            moved = east_flow([load(c) for c in range(3)], coef, x)
            for i in range(3):
                flow[3 * q + i, x] = moved[i]
        return carry

    lax.fori_loop(1, rows + 3, flows, 0)

    def last(x, carry):
        force = forcing(1, x, 1, LANE)
        applied = apply_row(lambda c, r: mid[c, r], lambda i, r: flow[6 + i, r], coef, x, LANE)
        scale = scale_ref[x, :, :LANE]
        for c in range(3):
            now = now_ref[pl.ds(c * lev * rows + x - 2, lev, stride=rows), :]
            current = mid[c, x, :, :LANE]
            mid_out[pl.ds(c * lev * rows + x - 2, lev, stride=rows), :] = current
            next_out[pl.ds(c * lev * rows + x - 2, lev, stride=rows), :] = (
                2.0 * current - now + scale * (applied[c] + force[c])
            )
        return carry

    lax.fori_loop(2, rows + 2, last, 0)


def specs(text):
    space = {"v": VMEM, "s": SMEM}
    return [pl.BlockSpec(memory_space=space[kind]) for kind in text]


def f32(*shape):
    return jax.ShapeDtypeStruct(shape, jnp.float32)


def neighbours(axis, step):
    count = lax.axis_size(axis)
    return [(i, i + step) for i in range(count) if 0 <= i + step < count]


def local(disp_now, disp_prev, density, moduli, coarse, block_route, ranges, offsets):
    _, lev, rows, north_cells = disp_now.shape
    groups = lev // 2
    c_east = (rows + 23) * 4 // 25 + 2
    c_north = (north_cells + 23) * 4 // 25 + 2
    block_hold = coarse.shape[0]
    samples = coarse.shape[1] // 6
    n_x = lax.axis_size("gx")
    n_y = lax.axis_size("gy")
    assert lev == 8 and north_cells == LANE and block_hold == 2
    assert (c_east, c_north) == (8, 26) and 6 * (rows + 4) <= LANE
    now, prev, dens, mods = (a.reshape(-1, north_cells) for a in (disp_now, disp_prev, density, moduli))
    wide = rows + 4

    payload, first, last = pl.pallas_call(
        functools.partial(pre_kernel, lev, rows, groups, samples),
        out_shape=(f32(n_x * n_y, 40, LANE), f32(15, lev, LANE), f32(15, lev, LANE)),
        in_specs=specs("vvvvvss"),
        out_specs=specs("vvv"),
        scratch_shapes=[VMEM((24, WIDE), jnp.float32)],
        name="pre",
    )(coarse, now, prev, dens, mods, offsets, ranges)
    got = lax.all_to_all(payload, ("gx", "gy"), split_axis=0, concat_axis=0, tiled=True)
    before = lax.ppermute(last, "gx", neighbours("gx", 1))
    after = lax.ppermute(first, "gx", neighbours("gx", -1))
    to_west, to_east, meta = pl.pallas_call(
        functools.partial(pack_kernel, lev, rows, groups),
        out_shape=(f32(4, lev, LANE), f32(4, lev, LANE), f32(lev, LANE)),
        in_specs=specs("vvvvvvss"),
        out_specs=specs("vvv"),
        cost_estimate=pl.CostEstimate(flops=2000000, bytes_accessed=1000000, transcendentals=0),
        name="pack",
    )(now, prev, dens, mods, before, after, offsets, ranges)
    west = lax.ppermute(to_east, "gy", neighbours("gy", 1))
    east = lax.ppermute(to_west, "gy", neighbours("gy", -1))
    place = jnp.stack([lax.axis_index("gx"), lax.axis_index("gy"), jnp.int32(n_y)]).astype(jnp.int32)
    prepared = pl.pallas_call(
        functools.partial(prep_kernel, lev, rows, groups, c_north),
        out_shape=(
            f32(2, wide, lev, WIDE),
            f32(3, wide, lev, WIDE),
            f32(wide, lev, WIDE),
            f32(2, 3, lev, WIDE),
            f32(3, 3, 2, lev, LANE),
            f32(3, lev, WIDE),
            jax.ShapeDtypeStruct((3, LANE, LANE), jnp.bfloat16),
            jax.ShapeDtypeStruct((3, WIDE, LANE), jnp.bfloat16),
            jax.ShapeDtypeStruct((9 * groups,), jnp.int32),
        ),
        in_specs=specs("vvvvvvvvvss"),
        out_specs=specs("vvvvvvvvs"),
        scratch_shapes=[
            VMEM((3, wide, lev, WIDE), jnp.float32),
            VMEM((3, wide, lev, WIDE), jnp.float32),
            VMEM((COEFS, wide, lev, WIDE), jnp.float32),
        ],
        cost_estimate=pl.CostEstimate(flops=10000000, bytes_accessed=3000000, transcendentals=0),
        name="prep",
    )(now, prev, dens, mods, before, after, west, east, meta, block_route, place)
    mods_x, base, scale, mask, level_w, shift, own_hat, side_hat, index = prepared
    incident, mid, nxt = pl.pallas_call(
        functools.partial(finish_kernel, lev, rows, groups, c_east, c_north, block_hold),
        out_shape=(
            f32(6 * lev * rows, LANE),
            f32(3 * lev * rows, LANE),
            f32(3 * lev * rows, LANE),
        ),
        in_specs=specs("vsvvvvvvvvv"),
        out_specs=specs("vvv"),
        scratch_shapes=[
            VMEM((c_east, 16, LANE), jnp.float32),
            VMEM((6 * c_east * lev, LANE), jnp.float32),
            VMEM((6 * c_east * lev, WIDE), jnp.float32),
            VMEM((3, 6 * c_east, lev, WIDE), jnp.float32),
            VMEM((12, wide, lev, WIDE), jnp.float32),
            VMEM((9, wide, lev, WIDE), jnp.float32),
            VMEM((3, wide, lev, WIDE), jnp.float32),
            VMEM((COEFS, wide, lev, WIDE), jnp.float32),
        ],
        cost_estimate=pl.CostEstimate(flops=20000000, bytes_accessed=6000000, transcendentals=0),
        name="finish",
    )(got, index, mods_x, base, scale, mask, level_w, shift, own_hat, side_hat, now)
    return (
        incident.reshape(2, 3, lev, rows, north_cells),
        mid.reshape(disp_now.shape),
        nxt.reshape(disp_now.shape),
    )


def solution(mesh):
    return jax.shard_map(
        local,
        mesh=mesh,
        in_specs=(
            P(None, None, "gx", "gy"),
            P(None, None, "gx", "gy"),
            P(None, "gx", "gy"),
            P(None, None, "gx", "gy"),
            P(("gx", "gy"), None, None),
            P(),
            P("gx", "gy", None),
            P("gx", "gy", None, None),
        ),
        out_specs=(
            P(None, None, None, "gx", "gy"),
            P(None, None, "gx", "gy"),
            P(None, None, "gx", "gy"),
        ),
        check_vma=False,
    )
```

```python
import functools

import jax
import jax.numpy as jnp
from jax import lax
from jax.experimental import pallas as pl
from jax.experimental.pallas import tpu as pltpu
from jax.sharding import PartitionSpec as P


step_square = 0.05
time_weights = ((-0.0595, 0.7735, 0.3315, -0.0455), (-0.063756, 0.607068, 0.517132, -0.060444))

LANE = 128
WIDE = 256
VMEM = pltpu.VMEM
SMEM = pltpu.SMEM


def lane_ids(shape):
    return lax.broadcasted_iota(jnp.int32, shape, len(shape) - 1)


def sub_ids(shape):
    return lax.broadcasted_iota(jnp.int32, shape, len(shape) - 2)


def shift_up(u):
    count = u.shape[0]
    return jnp.where(sub_ids(u.shape) == count - 1, 0.0, pltpu.roll(u, count - 1, 0))


def shift_down(u):
    return jnp.where(sub_ids(u.shape) == 0, 0.0, pltpu.roll(u, 1, 0))


def shift_next(u):
    return pltpu.roll(u, u.shape[1] - 1, 1)


def shift_prior(u):
    return pltpu.roll(u, 1, 1)


def level_row(ref, plane, levels, rows, r):
    return ref[pl.ds(plane * levels * rows + r, levels, stride=rows), :]


def rows_loop(start, stop, most, body):
    step = max(d for d in range(1, most + 1) if (stop - start) % d == 0)

    def chunk(i, carry):
        for r in range(step):
            body(start + i * step + r)
        return carry

    lax.fori_loop(0, (stop - start) // step, chunk, 0)


def meta_vector(off_ref, rng_ref, groups):
    shape = (8, LANE)
    lane = lane_ids(shape)
    out = jnp.zeros(shape, jnp.float32)
    for g in range(groups):
        for q in range(3):
            out = jnp.where(lane == 3 * g + q, off_ref[0, q, 0, g].astype(jnp.float32), out)
    for q in range(2):
        out = jnp.where(lane == 3 * groups + q, rng_ref[0, 0, q].astype(jnp.float32), out)
    return out


def pre_kernel(
    lev, rows, groups, samples, *refs
):
    sources, (off_ref, rng_ref, pay_ref, first_ref, last_ref, scr) = refs[:5], refs[5:11]
    held, sems = refs[11:16], refs[16]
    copies = [pltpu.make_async_copy(sources[i], held[i], sems.at[i]) for i in range(5)]
    for copy in copies:
        copy.start()
    coarse_ref, now_ref, prev_ref, dens_ref, mod_ref = held
    copies[0].wait()
    for k in range(coarse_ref.shape[0]):
        mixed = []
        for n in range(2):
            total = None
            for t in range(samples):
                term = time_weights[n][t] * coarse_ref[k, 6 * t : 6 * t + 6, :]
                total = term if total is None else total + term
            mixed.append(total)
        scr[8 * k : 8 * k + 6, :] = mixed[0]
        scr[8 * k + 6 : 8 * k + 8, :] = mixed[1][0:2]
        scr[16 + 4 * k : 20 + 4 * k, :] = mixed[1][2:6]
    head = [scr[8 * i : 8 * i + 8, :LANE] for i in range(3)]
    tail = [scr[8 * i : 8 * i + 8, LANE:] for i in range(3)]
    lane = lane_ids((8, LANE))
    tiles = head + [
        jnp.where(lane < 80, tail[0], pltpu.roll(tail[2], 80, 1)),
        jnp.where(lane < 80, tail[1], pltpu.roll(tail[2], 40, 1)),
    ]

    for i, tile in enumerate(tiles):
        pay_ref[8 * i : 8 * i + 8, :] = tile
    meta = meta_vector(off_ref, rng_ref, groups)
    for copy in copies[1:]:
        copy.wait()
    for ref, start, edge in ((first_ref, 0, 0), (last_ref, rows - 2, rows - 1)):
        for c in range(3):
            for r in range(2):
                ref[2 * c + r] = level_row(now_ref, c, lev, rows, start + r)
            ref[10 + c] = level_row(prev_ref, c, lev, rows, edge)
        for k in range(2):
            for r in range(2):
                ref[6 + 2 * k + r] = level_row(mod_ref, k, lev, rows, start + r)
        ref[13] = level_row(dens_ref, 0, lev, rows, edge)
        ref[14] = meta


def plane_row(refs, lev, rows, plane, x):
    now_ref, prev_ref, dens_ref, mod_ref, before_ref, after_ref = refs
    if plane < 3:
        source, own, strip, both = now_ref, plane, 2 * plane, True
    elif plane < 5:
        source, own, strip, both = mod_ref, plane - 3, 6 + 2 * (plane - 3), True
    elif plane < 8:
        source, own, strip, both = prev_ref, plane - 5, 10 + plane - 5, False
    else:
        source, own, strip, both = dens_ref, 0, 13, False
    if 2 <= x < rows + 2:
        return level_row(source, own, lev, rows, x - 2)
    ref, r = (before_ref, x) if x < 2 else (after_ref, x - rows - 2)
    if both:
        return ref[strip + r]
    return ref[strip] if x in (1, rows + 2) else None


def pack_kernel(
    lev, rows, groups, now_ref, prev_ref, dens_ref, mod_ref, before_ref, after_ref, off_ref, rng_ref,
    west_ref, east_ref, meta_ref
):
    refs = (now_ref, prev_ref, dens_ref, mod_ref, before_ref, after_ref)
    lane = lane_ids((lev, LANE))
    span = 2 * (rows + 4)
    for block in range(3):
        west = jnp.zeros((lev, LANE), jnp.float32)
        east = jnp.zeros((lev, LANE), jnp.float32)
        for p in range(3):
            for x in range(rows + 4):
                v = plane_row(refs, lev, rows, 3 * block + p, x)
                if v is None:
                    continue
                at = span * p + 2 * x
                here = (lane == at) | (lane == at + 1)
                west = jnp.where(here, pltpu.roll(v, at, 1), west)
                east = jnp.where(here, pltpu.roll(v, (at + 2) % LANE, 1), east)
        west_ref[block] = west
        east_ref[block] = east
    sub = sub_ids((lev, LANE))
    meta = meta_vector(off_ref, rng_ref, groups)
    both = jnp.where(sub == 0, before_ref[14], jnp.where(sub == 1, meta, after_ref[14]))
    west_ref[3] = both
    east_ref[3] = both
    meta_ref[...] = both


MU = {"l+": 0, "l-": 1, "e+": 2, "e-": 3, "n+": 4, "n-": 5}
STIFF = {"l+": 6, "l-": 7, "e+": 8, "e-": 9, "n+": 10, "n-": 11}
CENTER = 12
MU_QUARTER = 15
LAME_QUARTER = 16
COEFS = 17


def quarter_row(mod_ref, coef_ref, x):
    coef_ref[MU_QUARTER, x] = 0.25 * mod_ref[0, x]
    coef_ref[LAME_QUARTER, x] = 0.25 * mod_ref[1, x]


def coef_row(mod_ref, coef_ref, x):
    sums = []
    for stiff, table in ((False, MU), (True, STIFF)):

        def half(r):
            mu = mod_ref[0, r]
            return 0.5 * mod_ref[1, r] + mu if stiff else 0.5 * mu

        k = half(x)
        values = {
            "l+": k + shift_up(k),
            "l-": k + shift_down(k),
            "e+": k + half(x + 1),
            "e-": k + half(x - 1),
            "n+": k + shift_next(k),
            "n-": k + shift_prior(k),
        }
        for name, value in values.items():
            coef_ref[table[name], x] = value
        sums.append({d: values[d + "+"] + values[d + "-"] for d in "len"})
    soft, hard = sums
    coef_ref[CENTER + 0, x] = hard["l"] + soft["e"] + soft["n"]
    coef_ref[CENTER + 1, x] = soft["l"] + hard["e"] + soft["n"]
    coef_ref[CENTER + 2, x] = soft["l"] + soft["e"] + hard["n"]


def east_flow(u, coef_ref, x):
    mu = coef_ref[MU_QUARTER, x]
    lame = coef_ref[LAME_QUARTER, x]
    rise = [shift_up(u[c]) - shift_down(u[c]) for c in range(2)]
    run = [shift_next(u[c]) - shift_prior(u[c]) for c in (1, 2)]
    return mu * rise[1], lame * (rise[0] + run[1]), mu * run[0]


def apply_row(field, flow, coef_ref, x, width):
    def cut(v):
        return v[:, :width]

    u = [field(c, x) for c in range(3)]
    after = [field(c, x + 1) for c in range(3)]
    before = [field(c, x - 1) for c in range(3)]
    up = [shift_up(v) for v in u]
    down = [shift_down(v) for v in u]
    nxt = [shift_next(v) for v in u]
    prior = [shift_prior(v) for v in u]
    d_l = [up[c] - down[c] for c in range(3)]
    d_n = [nxt[c] - prior[c] for c in range(3)]
    d_e = [after[c] - before[c] for c in range(3)]
    mu = coef_ref[MU_QUARTER, x]
    lame = coef_ref[LAME_QUARTER, x]
    level_flow = (cut(lame * (d_e[1] + d_n[2])), cut(mu * d_e[0]), cut(mu * d_n[0]))
    north_flow = (mu * d_l[2], mu * d_e[2], lame * (d_l[0] + d_e[1]))
    out = []
    for i in range(3):

        def coef(name):
            table = STIFF if "len".index(name[0]) == i else MU
            return cut(coef_ref[table[name], x])

        total = cut(flow(i, x + 1)) - cut(flow(i, x - 1))
        total += shift_up(level_flow[i]) - shift_down(level_flow[i])
        total += cut(shift_next(north_flow[i]) - shift_prior(north_flow[i]))
        total += coef("l+") * cut(up[i]) + coef("l-") * cut(down[i])
        total += coef("e+") * cut(after[i]) + coef("e-") * cut(before[i])
        total += coef("n+") * cut(nxt[i]) + coef("n-") * cut(prior[i])
        total -= cut(coef_ref[CENTER + i, x]) * cut(u[i])
        out.append(total)
    return out


def prep_kernel(
    lev, rows, groups, c_north, n_x, n_y, now_ref, prev_ref, dens_ref, mod_ref, before_ref, after_ref, west_ref, east_ref, meta_ref,
    route_ref, place_ref, mods_ref, base_ref, scale_ref, mask_ref, level_ref, shift_ref, own_hat_ref, side_hat_ref,
    index_ref, now_x, flow, coef
):
    refs = (now_ref, prev_ref, dens_ref, mod_ref, before_ref, after_ref)
    lane = lane_ids((lev, LANE))
    sub = sub_ids((lev, LANE))
    span = 2 * (rows + 4)
    metas = (meta_ref[...], east_ref[3], west_ref[3])

    for i in range(9 * groups):
        index_ref[i] = 0
    my_x, my_y = place_ref[0], place_ref[1]
    half = n_x * n_y // 2
    upper = (2 * my_x >= n_x).astype(jnp.int32)

    def find(b, carry):
        slot = route_ref[b]
        tile = lax.div(slot, groups)
        g = slot - tile * groups
        tile_x = lax.div(tile, n_y)
        d_x = tile_x - my_x + 1
        d_y = tile - tile_x * n_y - my_y
        column = jnp.where(d_y < 0, 2, d_y)

        @pl.when((d_x >= 0) & (d_x < 3) & (d_y >= -1) & (d_y < 2))
        def _():
            source = lax.div(b, 2)
            far = (source >= half).astype(jnp.int32)
            seat = 2 * (source - far * half) + (far ^ upper)
            index_ref[(d_x * 3 + column) * groups + g] = 2 * seat + b - 2 * source

        return carry

    lax.fori_loop(0, route_ref.shape[0], find, 0)

    def sides(plane, x):
        block, p = divmod(plane, 3)
        at = span * p + 2 * x
        return jnp.where(
            lane < 2,
            pltpu.roll(east_ref[block], (-at) % LANE, 1),
            jnp.where(lane >= LANE - 2, pltpu.roll(west_ref[block], (LANE - 2 - at) % LANE, 1), 0.0),
        )

    for x in range(rows + 4):
        for c in range(3):
            now_x[c, x, :, :LANE] = plane_row(refs, lev, rows, c, x)
            now_x[c, x, :, LANE:] = sides(c, x)
        for k in range(2):
            mods_ref[k, x, :, :LANE] = plane_row(refs, lev, rows, 3 + k, x)
            mods_ref[k, x, :, LANE:] = sides(3 + k, x)
        if 1 <= x < rows + 3:
            for c in range(3):
                base_ref[c, x, :, :LANE] = plane_row(refs, lev, rows, 5 + c, x)
                base_ref[c, x, :, LANE:] = sides(5 + c, x)
            for part, v in ((slice(0, LANE), plane_row(refs, lev, rows, 8, x)), (slice(LANE, WIDE), sides(8, x))):
                there = v > 0.0
                scale_ref[x, :, part] = jnp.where(there, step_square / jnp.where(there, v, 1.0), 0.0)

    def first(x):
        quarter_row(mods_ref, coef, x)
        parts = east_flow([now_x[c, x] for c in range(3)], coef, x)
        for i in range(3):
            flow[i, x] = parts[i]

    rows_loop(0, rows + 4, 5, first)
    rows_loop(1, rows + 3, 6, lambda x: coef_row(mods_ref, coef, x))

    def second(x):
        applied = apply_row(lambda c, r: now_x[c, r], lambda i, r: flow[i, r], coef, x, WIDE)
        for c in range(3):
            base_ref[c, x] = 2.0 * now_x[c, x] - base_ref[c, x] + scale_ref[x] * applied[c]

    rows_loop(1, rows + 3, 3, second)

    group_of_sub = sub // 2
    second_level = (sub - 2 * group_of_sub).astype(jnp.float32)
    k_row = sub_ids((LANE, LANE))
    k_lane = lane_ids((LANE, LANE))
    sub_f = sub.astype(jnp.float32)
    for t in range(3):
        def entry(column, i):
            return metas[column][t : t + 1, i : i + 1]

        for column in range(3):
            low = entry(column, 3 * groups)
            high = entry(column, 3 * groups + 1)
            outer = (sub_f < low).astype(jnp.float32)
            inner = ((sub_f >= low) & (sub_f < high)).astype(jnp.float32)
            if column == 0:
                mask_ref[0, t, :, :LANE] = outer
                mask_ref[1, t, :, :LANE] = inner
            elif column == 1:
                east_masks = (outer, inner)
            else:
                for q, own in enumerate((outer, inner)):
                    mask_ref[q, t, :, LANE:] = jnp.where(lane < LANE // 2, east_masks[q], own)
            depth = second_level
            east_at = jnp.zeros((lev, LANE), jnp.float32)
            hold = jnp.zeros((lev, LANE), jnp.float32)
            north_at = jnp.zeros((LANE, LANE), jnp.float32)
            point = jnp.zeros((LANE, LANE), jnp.float32)
            for g in range(groups):
                here = group_of_sub == g
                depth = jnp.where(here, second_level + entry(column, 3 * g), depth)
                east_at = jnp.where(here, 4.0 * entry(column, 3 * g + 1), east_at)
                mine = here & (lane >= g * c_north) & (lane < (g + 1) * c_north)
                hold = jnp.where(mine & (high > 2.0 * g + 1.0), 1.0 / 625.0, hold)
                there = (k_row >= g * c_north) & (k_row < (g + 1) * c_north)
                north_at = jnp.where(there, 4.0 * entry(column, 3 * g + 2), north_at)
                point = jnp.where(there, 25.0 * (k_row - g * c_north).astype(jnp.float32), point)
            depth = depth * (4.0 / 25.0)
            level_ref[t, column, 0] = hold * (1.0 - depth)
            level_ref[t, column, 1] = hold * depth
            hat = jnp.maximum(25.0 - jnp.abs(north_at + 4.0 * k_lane.astype(jnp.float32) - point), 0.0)
            hat = jnp.where(k_row < groups * c_north, hat, 0.0)
            if column == 0:
                shift_ref[t, :, :LANE] = east_at
                own_hat_ref[t] = hat.astype(jnp.bfloat16)
            elif column == 1:
                east_shift = east_at
                side_hat_ref[t, :LANE, :] = jnp.where(k_lane < LANE // 2, hat, 0.0).astype(jnp.bfloat16)
            else:
                shift_ref[t, :, LANE:] = jnp.where(lane < LANE // 2, east_shift, east_at)
                side_hat_ref[t, LANE:, :] = jnp.where(k_lane >= LANE // 2, hat, 0.0).astype(jnp.bfloat16)


def split_dot(ref, hat):
    v = ref[...]
    high = v.astype(jnp.bfloat16)
    low = (v - high.astype(jnp.float32)).astype(jnp.bfloat16)
    return jnp.dot(high, hat, preferred_element_type=jnp.float32) + jnp.dot(
        low, hat, preferred_element_type=jnp.float32
    )


def finish_kernel(
    lev, rows, groups, c_east, c_north, got_ref, index_ref, mods_ref, base_ref, scale_ref, mask_ref,
    level_ref, shift_ref, own_hat_ref, side_hat_ref, now_ref, inc_out, mid_out, next_out,
    mixed, own_rows, side_rows, north, parts, flow, mid, coef
):
    lane = lane_ids((8, LANE))
    rows_loop(0, rows + 4, 5, lambda x: quarter_row(mods_ref, coef, x))
    rows_loop(1, rows + 3, 6, lambda x: coef_row(mods_ref, coef, x))

    def tile_row(t, carry):
        for column in range(3):
            pieces = []
            for g in range(groups):
                b = index_ref[(t * 3 + column) * groups + g]
                source = b >> 1
                k = b & 1
                top = pl.multiple_of(8 * k, 8)
                third = got_ref[source, 24:32, :]
                fourth = got_ref[source, 32:40, :]
                tail = jnp.where(lane < 40, pltpu.roll(third, LANE - 80, 1), pltpu.roll(fourth, LANE - 40, 1))
                pieces.append(
                    (
                        (got_ref[source, pl.ds(top, 8), :], got_ref[source, pl.ds(24 + top, 8), :]),
                        (pltpu.roll(got_ref[source, 16:24, :], 4 * k, 0), pltpu.roll(tail, 4 * k, 0)),
                    )
                )
            for a in range(c_east):
                start = a * c_north
                for half in range(2):
                    total = jnp.zeros((8, LANE), jnp.float32)
                    for g in range(groups):
                        body, tail = pieces[g][half]
                        at = g * c_north
                        if start + c_north <= LANE:
                            moved = pltpu.roll(body, (at - start) % LANE, 1)
                        elif start >= LANE:
                            moved = pltpu.roll(tail, (at - start) % LANE, 1)
                        else:
                            moved = jnp.where(
                                lane < at + LANE - start,
                                pltpu.roll(body, (at - start) % LANE, 1),
                                pltpu.roll(tail, (at - start) % LANE, 1),
                            )
                        total = jnp.where((lane >= at) & (lane < at + c_north), moved, total)
                    mixed[a, 8 * half : 8 * half + 8, :] = total
            w0 = level_ref[t, column, 0]
            w1 = level_ref[t, column, 1]
            for nc in range(6):
                r = (nc // 3) * 6 + 2 * (nc % 3)
                for a in range(c_east):
                    value = w0 * jnp.broadcast_to(mixed[a, r : r + 1, :], (lev, LANE)) + w1 * jnp.broadcast_to(
                        mixed[a, r + 1 : r + 2, :], (lev, LANE)
                    )
                    at = (nc * c_east + a) * lev
                    if column == 0:
                        own_rows[at : at + lev, :] = value
                    elif column == 1:
                        side_rows[at : at + lev, :LANE] = value
                    else:
                        side_rows[at : at + lev, LANE:] = value
        own = split_dot(own_rows, own_hat_ref[t])
        north[t, :, :, :LANE] = own.reshape(6 * c_east, lev, LANE)
        side = split_dot(side_rows, side_hat_ref[t])
        north[t, :, :, LANE:] = side.reshape(6 * c_east, lev, LANE)
        return carry

    lax.fori_loop(0, 3, tile_row, 0)

    near = (4 * 24) // 25 + 3

    def east(x, t, cell):
        first = 4 * cell // 25 if isinstance(cell, int) else lax.div(4 * cell, 25)
        ahead = 4 * cell - 25 * first
        at = shift_ref[t] + (float(ahead) if isinstance(cell, int) else ahead.astype(jnp.float32))
        weights = [jnp.maximum(25.0 - jnp.abs(at - 25.0 * i), 0.0) for i in range(near)]
        outer = mask_ref[0, t]
        inner = mask_ref[1, t]
        values = []
        for nc in range(6):
            total = None
            for i in range(near):
                term = weights[i] * north[t, nc * c_east + first + i]
                total = term if total is None else total + term
            values.append(total)
            parts[nc, x] = outer * total
            parts[6 + nc, x] = inner * total
            if not isinstance(cell, int):
                inc_out[pl.ds(nc * lev * rows + cell, lev, stride=rows), :] = total[:, :LANE]
        for q, mask in enumerate((outer, inner)):
            moved = east_flow([mask * values[c] for c in range(3)], coef, x)
            for i in range(3):
                flow[3 * q + i, x] = moved[i]

    rows_loop(0, rows, 4, lambda cell: east(cell + 2, 1, cell))
    for r in range(2):
        east(r, 0, rows - 2 + r)
        east(rows + 2 + r, 2, r)

    def forcing(step, x, t, width):
        outside = apply_row(
            lambda c, r: parts[3 * step + c, r], lambda i, r: flow[i, r], coef, x, width
        )
        inside = apply_row(
            lambda c, r: parts[6 + 3 * step + c, r], lambda i, r: flow[3 + i, r], coef, x, width
        )
        outer = mask_ref[0, t][:, :width]
        inner = mask_ref[1, t][:, :width]
        return [inner * outside[c] - outer * inside[c] for c in range(3)]

    def middle(x):
        t = (x >= 2).astype(jnp.int32) + (x >= rows + 2).astype(jnp.int32)
        force = forcing(0, x, t, WIDE)
        for c in range(3):
            mid[c, x] = base_ref[c, x] + scale_ref[x] * force[c]

    rows_loop(1, rows + 3, 3, middle)

    def flows(x):
        for q, load in enumerate(
            (lambda c: parts[3 + c, x], lambda c: parts[9 + c, x], lambda c: mid[c, x])
        ):
            moved = east_flow([load(c) for c in range(3)], coef, x)
            for i in range(3):
                flow[3 * q + i, x] = moved[i]

    rows_loop(1, rows + 3, 6, flows)

    def last(x):
        force = forcing(1, x, 1, LANE)
        applied = apply_row(lambda c, r: mid[c, r], lambda i, r: flow[6 + i, r], coef, x, LANE)
        scale = scale_ref[x, :, :LANE]
        for c in range(3):
            now = now_ref[pl.ds(c * lev * rows + x - 2, lev, stride=rows), :]
            current = mid[c, x, :, :LANE]
            mid_out[pl.ds(c * lev * rows + x - 2, lev, stride=rows), :] = current
            next_out[pl.ds(c * lev * rows + x - 2, lev, stride=rows), :] = (
                2.0 * current - now + scale * (applied[c] + force[c])
            )

    rows_loop(2, rows + 2, 4, last)


def specs(text):
    space = {"v": VMEM, "s": SMEM, "h": pltpu.HBM}
    return [pl.BlockSpec(memory_space=space[kind]) for kind in text]


def f32(*shape):
    return jax.ShapeDtypeStruct(shape, jnp.float32)


def neighbours(axis, step):
    count = lax.axis_size(axis)
    return [(i, i + step) for i in range(count) if 0 <= i + step < count]


def local(disp_now, disp_prev, density, moduli, coarse, block_route, ranges, offsets):
    _, lev, rows, north_cells = disp_now.shape
    groups = lev // 2
    c_east = (rows + 23) * 4 // 25 + 2
    c_north = (north_cells + 23) * 4 // 25 + 2
    block_hold = coarse.shape[0]
    samples = coarse.shape[1] // 6
    n_x = lax.axis_size("gx")
    n_y = lax.axis_size("gy")
    assert lev == 8 and north_cells == LANE and block_hold == 2
    assert (c_east, c_north) == (8, 26) and 6 * (rows + 4) <= LANE
    now, prev, dens, mods = (a.reshape(-1, north_cells) for a in (disp_now, disp_prev, density, moduli))
    wide = rows + 4
    shifts = offsets.transpose(0, 3, 1, 2)
    limit = pltpu.CompilerParams(vmem_limit_bytes=16 * 2**20)
    assert n_x % 2 == 0

    payload, first, last = pl.pallas_call(
        functools.partial(pre_kernel, lev, rows, groups, samples),
        out_shape=(f32(40, LANE), f32(15, lev, LANE), f32(15, lev, LANE)),
        in_specs=specs("hhhhhss"),
        out_specs=specs("vvv"),
        scratch_shapes=[VMEM((24, WIDE), jnp.float32)]
        + [VMEM(a.shape, jnp.float32) for a in (coarse, now, prev, dens, mods)]
        + [pltpu.SemaphoreType.DMA((5,))],
        compiler_params=limit,
        name="pre",
    )(*(pltpu.with_memory_space_constraint(a, pltpu.HBM) for a in (coarse, now, prev, dens, mods, shifts, ranges)))
    half = n_x * n_y // 2
    twin = lax.ppermute(payload, "gx", [(i, (i + n_x // 2) % n_x) for i in range(n_x)])
    before = lax.ppermute(last, "gx", neighbours("gx", 1))
    after = lax.ppermute(first, "gx", neighbours("gx", -1))
    chunk = jnp.concatenate([payload, twin], axis=0)
    got = lax.all_to_all(
        jnp.broadcast_to(chunk[None], (half,) + chunk.shape),
        ("gx", "gy"),
        split_axis=0,
        concat_axis=0,
        tiled=True,
        axis_index_groups=[list(range(half)), list(range(half, 2 * half))],
    ).reshape(2 * half, 40, LANE)
    to_west, to_east, meta = pl.pallas_call(
        functools.partial(pack_kernel, lev, rows, groups),
        out_shape=(f32(4, lev, LANE), f32(4, lev, LANE), f32(lev, LANE)),
        in_specs=specs("vvvvvvss"),
        out_specs=specs("vvv"),
        cost_estimate=pl.CostEstimate(flops=2000000, bytes_accessed=1000000, transcendentals=0),
        compiler_params=limit,
        name="pack",
    )(now, prev, dens, mods, before, after, shifts, ranges)
    west = lax.ppermute(to_east, "gy", neighbours("gy", 1))
    east = lax.ppermute(to_west, "gy", neighbours("gy", -1))
    place = jnp.stack([lax.axis_index("gx"), lax.axis_index("gy")]).astype(jnp.int32)
    prepared = pl.pallas_call(
        functools.partial(prep_kernel, lev, rows, groups, c_north, n_x, n_y),
        out_shape=(
            f32(2, wide, lev, WIDE),
            f32(3, wide, lev, WIDE),
            f32(wide, lev, WIDE),
            f32(2, 3, lev, WIDE),
            f32(3, 3, 2, lev, LANE),
            f32(3, lev, WIDE),
            jax.ShapeDtypeStruct((3, LANE, LANE), jnp.bfloat16),
            jax.ShapeDtypeStruct((3, WIDE, LANE), jnp.bfloat16),
            jax.ShapeDtypeStruct((9 * groups,), jnp.int32),
        ),
        in_specs=specs("vvvvvvvvvss"),
        out_specs=specs("vvvvvvvvs"),
        scratch_shapes=[
            VMEM((3, wide, lev, WIDE), jnp.float32),
            VMEM((3, wide, lev, WIDE), jnp.float32),
            VMEM((COEFS, wide, lev, WIDE), jnp.float32),
        ],
        cost_estimate=pl.CostEstimate(flops=10000000, bytes_accessed=3000000, transcendentals=0),
        compiler_params=limit,
        name="prep",
    )(now, prev, dens, mods, before, after, west, east, meta, block_route, place)
    mods_x, base, scale, mask, level_w, shift, own_hat, side_hat, index = prepared
    incident, mid, nxt = pl.pallas_call(
        functools.partial(finish_kernel, lev, rows, groups, c_east, c_north),
        out_shape=(
            f32(6 * lev * rows, LANE),
            f32(3 * lev * rows, LANE),
            f32(3 * lev * rows, LANE),
        ),
        in_specs=specs("vsvvvvvvvvv"),
        out_specs=specs("vvv"),
        scratch_shapes=[
            VMEM((c_east, 16, LANE), jnp.float32),
            VMEM((6 * c_east * lev, LANE), jnp.float32),
            VMEM((6 * c_east * lev, WIDE), jnp.float32),
            VMEM((3, 6 * c_east, lev, WIDE), jnp.float32),
            VMEM((12, wide, lev, WIDE), jnp.float32),
            VMEM((9, wide, lev, WIDE), jnp.float32),
            VMEM((3, wide, lev, WIDE), jnp.float32),
            VMEM((COEFS, wide, lev, WIDE), jnp.float32),
        ],
        cost_estimate=pl.CostEstimate(flops=20000000, bytes_accessed=6000000, transcendentals=0),
        compiler_params=limit,
        name="finish",
    )(got, index, mods_x, base, scale, mask, level_w, shift, own_hat, side_hat, now)
    return (
        incident.reshape(2, 3, lev, rows, north_cells),
        mid.reshape(disp_now.shape),
        nxt.reshape(disp_now.shape),
    )


def solution(mesh):
    return jax.shard_map(
        local,
        mesh=mesh,
        in_specs=(
            P(None, None, "gx", "gy"),
            P(None, None, "gx", "gy"),
            P(None, "gx", "gy"),
            P(None, None, "gx", "gy"),
            P(("gx", "gy"), None, None),
            P(),
            P("gx", "gy", None),
            P("gx", "gy", None, None),
        ),
        out_specs=(
            P(None, None, None, "gx", "gy"),
            P(None, None, "gx", "gy"),
            P(None, None, "gx", "gy"),
        ),
        check_vma=False,
    )
```

```python
import functools

import jax
import jax.numpy as jnp
from jax import lax
from jax.experimental import pallas as pl
from jax.experimental.pallas import tpu as pltpu
from jax.sharding import PartitionSpec as P


step_square = 0.05
time_weights = ((-0.0595, 0.7735, 0.3315, -0.0455), (-0.063756, 0.607068, 0.517132, -0.060444))

LANE = 128
WIDE = 256
VMEM = pltpu.VMEM
SMEM = pltpu.SMEM


def lane_ids(shape):
    return lax.broadcasted_iota(jnp.int32, shape, len(shape) - 1)


def sub_ids(shape):
    return lax.broadcasted_iota(jnp.int32, shape, len(shape) - 2)


def shift_up(u):
    count = u.shape[0]
    return jnp.where(sub_ids(u.shape) == count - 1, 0.0, pltpu.roll(u, count - 1, 0))


def shift_down(u):
    return jnp.where(sub_ids(u.shape) == 0, 0.0, pltpu.roll(u, 1, 0))


def shift_next(u):
    return pltpu.roll(u, u.shape[1] - 1, 1)


def shift_prior(u):
    return pltpu.roll(u, 1, 1)


def level_row(ref, plane, levels, rows, r):
    return ref[pl.ds(plane * levels * rows + r, levels, stride=rows), :]


def rows_loop(start, stop, most, body):
    step = max(d for d in range(1, most + 1) if (stop - start) % d == 0)

    def chunk(i, carry):
        for r in range(step):
            body(start + i * step + r)
        return carry

    lax.fori_loop(0, (stop - start) // step, chunk, 0)


def quotient(v, n):
    return v >> (n.bit_length() - 1) if n & (n - 1) == 0 else lax.div(v, n)


def meta_vector(off_ref, rng_ref, groups):
    shape = (8, LANE)
    lane = lane_ids(shape)
    out = jnp.zeros(shape, jnp.float32)
    for g in range(groups):
        for q in range(3):
            out = jnp.where(lane == 3 * g + q, off_ref[0, q, 0, g].astype(jnp.float32), out)
    for q in range(2):
        out = jnp.where(lane == 3 * groups + q, rng_ref[0, 0, q].astype(jnp.float32), out)
    return out


def pre_kernel(
    lev, rows, groups, samples, *refs
):
    sources, (off_ref, rng_ref, pay_ref, first_ref, last_ref, scr) = refs[:5], refs[5:11]
    held, sems = refs[11:16], refs[16]
    copies = [pltpu.make_async_copy(sources[i], held[i], sems.at[i]) for i in range(5)]
    for copy in copies:
        copy.start()
    coarse_ref, now_ref, prev_ref, dens_ref, mod_ref = held
    copies[0].wait()
    for k in range(coarse_ref.shape[0]):
        mixed = []
        for n in range(2):
            total = None
            for t in range(samples):
                term = time_weights[n][t] * coarse_ref[k, 6 * t : 6 * t + 6, :]
                total = term if total is None else total + term
            mixed.append(total)
        scr[8 * k : 8 * k + 6, :] = mixed[0]
        scr[8 * k + 6 : 8 * k + 8, :] = mixed[1][0:2]
        scr[16 + 4 * k : 20 + 4 * k, :] = mixed[1][2:6]
    head = [scr[8 * i : 8 * i + 8, :LANE] for i in range(3)]
    tail = [scr[8 * i : 8 * i + 8, LANE:] for i in range(3)]
    lane = lane_ids((8, LANE))
    tiles = head + [
        jnp.where(lane < 80, tail[0], pltpu.roll(tail[2], 80, 1)),
        jnp.where(lane < 80, tail[1], pltpu.roll(tail[2], 40, 1)),
    ]

    for i, tile in enumerate(tiles):
        pay_ref[8 * i : 8 * i + 8, :] = tile
    meta = meta_vector(off_ref, rng_ref, groups)
    for copy in copies[1:]:
        copy.wait()
    for ref, start, edge in ((first_ref, 0, 0), (last_ref, rows - 2, rows - 1)):
        for c in range(3):
            for r in range(2):
                ref[2 * c + r] = level_row(now_ref, c, lev, rows, start + r)
            ref[10 + c] = level_row(prev_ref, c, lev, rows, edge)
        for k in range(2):
            for r in range(2):
                ref[6 + 2 * k + r] = level_row(mod_ref, k, lev, rows, start + r)
        ref[13] = level_row(dens_ref, 0, lev, rows, edge)
        ref[14] = meta


def plane_row(refs, lev, rows, plane, x):
    now_ref, prev_ref, dens_ref, mod_ref, before_ref, after_ref = refs
    if plane < 3:
        source, own, strip, both = now_ref, plane, 2 * plane, True
    elif plane < 5:
        source, own, strip, both = mod_ref, plane - 3, 6 + 2 * (plane - 3), True
    elif plane < 8:
        source, own, strip, both = prev_ref, plane - 5, 10 + plane - 5, False
    else:
        source, own, strip, both = dens_ref, 0, 13, False
    if 2 <= x < rows + 2:
        return level_row(source, own, lev, rows, x - 2)
    ref, r = (before_ref, x) if x < 2 else (after_ref, x - rows - 2)
    if both:
        return ref[strip + r]
    return ref[strip] if x in (1, rows + 2) else None


def pack_kernel(
    lev, rows, now_ref, prev_ref, dens_ref, mod_ref, before_ref, after_ref, own_ref,
    west_ref, east_ref, meta_ref
):
    refs = (now_ref, prev_ref, dens_ref, mod_ref, before_ref, after_ref)
    lane = lane_ids((lev, LANE))
    span = 2 * (rows + 4)
    for block in range(3):
        west = jnp.zeros((lev, LANE), jnp.float32)
        east = jnp.zeros((lev, LANE), jnp.float32)
        for p in range(3):
            for x in range(rows + 4):
                v = plane_row(refs, lev, rows, 3 * block + p, x)
                if v is None:
                    continue
                at = span * p + 2 * x
                here = (lane == at) | (lane == at + 1)
                west = jnp.where(here, pltpu.roll(v, at, 1), west)
                east = jnp.where(here, pltpu.roll(v, (at + 2) % LANE, 1), east)
        west_ref[block] = west
        east_ref[block] = east
    sub = sub_ids((lev, LANE))
    both = jnp.where(sub == 0, before_ref[14], jnp.where(sub == 1, own_ref[14], after_ref[14]))
    west_ref[3] = both
    east_ref[3] = both
    meta_ref[...] = both


MU = {"l+": 0, "l-": 1, "e+": 2, "e-": 3, "n+": 4, "n-": 5}
STIFF = {"l+": 6, "l-": 7, "e+": 8, "e-": 9, "n+": 10, "n-": 11}
CENTER = 12
MU_QUARTER = 15
LAME_QUARTER = 16
COEFS = 17


def quarter_row(mod_ref, coef_ref, x):
    coef_ref[MU_QUARTER, x] = 0.25 * mod_ref[0, x]
    coef_ref[LAME_QUARTER, x] = 0.25 * mod_ref[1, x]


def coef_row(mod_ref, coef_ref, x):
    sums = []
    for stiff, table in ((False, MU), (True, STIFF)):

        def half(r):
            mu = mod_ref[0, r]
            return 0.5 * mod_ref[1, r] + mu if stiff else 0.5 * mu

        k = half(x)
        values = {
            "l+": k + shift_up(k),
            "l-": k + shift_down(k),
            "e+": k + half(x + 1),
            "e-": k + half(x - 1),
            "n+": k + shift_next(k),
            "n-": k + shift_prior(k),
        }
        for name, value in values.items():
            coef_ref[table[name], x] = value
        sums.append({d: values[d + "+"] + values[d + "-"] for d in "len"})
    soft, hard = sums
    coef_ref[CENTER + 0, x] = hard["l"] + soft["e"] + soft["n"]
    coef_ref[CENTER + 1, x] = soft["l"] + hard["e"] + soft["n"]
    coef_ref[CENTER + 2, x] = soft["l"] + soft["e"] + hard["n"]


def east_flow(u, coef_ref, x):
    mu = coef_ref[MU_QUARTER, x]
    lame = coef_ref[LAME_QUARTER, x]
    rise = [shift_up(u[c]) - shift_down(u[c]) for c in range(2)]
    run = [shift_next(u[c]) - shift_prior(u[c]) for c in (1, 2)]
    return mu * rise[1], lame * (rise[0] + run[1]), mu * run[0]


def apply_row(field, flow, coef_ref, x, width):
    def cut(v):
        return v[:, :width]

    u = [field(c, x) for c in range(3)]
    after = [field(c, x + 1) for c in range(3)]
    before = [field(c, x - 1) for c in range(3)]
    up = [shift_up(v) for v in u]
    down = [shift_down(v) for v in u]
    nxt = [shift_next(v) for v in u]
    prior = [shift_prior(v) for v in u]
    d_l = [up[c] - down[c] for c in range(3)]
    d_n = [nxt[c] - prior[c] for c in range(3)]
    d_e = [after[c] - before[c] for c in range(3)]
    mu = coef_ref[MU_QUARTER, x]
    lame = coef_ref[LAME_QUARTER, x]
    level_flow = (cut(lame * (d_e[1] + d_n[2])), cut(mu * d_e[0]), cut(mu * d_n[0]))
    north_flow = (mu * d_l[2], mu * d_e[2], lame * (d_l[0] + d_e[1]))
    out = []
    for i in range(3):

        def coef(name):
            table = STIFF if "len".index(name[0]) == i else MU
            return cut(coef_ref[table[name], x])

        total = cut(flow(i, x + 1)) - cut(flow(i, x - 1))
        total += shift_up(level_flow[i]) - shift_down(level_flow[i])
        total += cut(shift_next(north_flow[i]) - shift_prior(north_flow[i]))
        total += coef("l+") * cut(up[i]) + coef("l-") * cut(down[i])
        total += coef("e+") * cut(after[i]) + coef("e-") * cut(before[i])
        total += coef("n+") * cut(nxt[i]) + coef("n-") * cut(prior[i])
        total -= cut(coef_ref[CENTER + i, x]) * cut(u[i])
        out.append(total)
    return out


def index_kernel(groups, n_x, n_y, route_ref, place_ref, index_ref):
    my_x, my_y = place_ref[0], place_ref[1]
    for i in range(9 * groups):
        index_ref[i] = 0
    half = n_x * n_y // 2
    upper = (2 * my_x >= n_x).astype(jnp.int32)

    def find(b):
        slot = route_ref[b]
        tile = quotient(slot, groups)
        tile_x = quotient(tile, n_y)
        d_x = tile_x - my_x + 1
        d_y = tile - tile_x * n_y - my_y
        column = jnp.where(d_y < 0, 2, d_y)
        near = (d_x >= 0) & (d_x < 3) & (d_y >= -1) & (d_y < 2)
        at = jnp.where(near, (d_x * 3 + column) * groups + slot - tile * groups, 9 * groups)
        source = quotient(b, 2)
        far = (source >= half).astype(jnp.int32)
        seat = 2 * (source - far * half) + (far ^ upper)
        index_ref[at] = 2 * seat + b - 2 * source

    rows_loop(0, route_ref.shape[0], 16, find)


def prep_kernel(
    lev, rows, groups, c_north, now_ref, prev_ref, dens_ref, mod_ref, before_ref, after_ref, west_ref, east_ref, meta_ref,
    mods_ref, base_ref, scale_ref, mask_ref, level_ref, shift_ref, own_hat_ref, side_hat_ref,
    now_x, flow, coef
):
    refs = (now_ref, prev_ref, dens_ref, mod_ref, before_ref, after_ref)
    lane = lane_ids((lev, LANE))
    sub = sub_ids((lev, LANE))
    span = 2 * (rows + 4)

    metas = (meta_ref[...], east_ref[3], west_ref[3])

    def sides(plane, x):
        block, p = divmod(plane, 3)
        at = span * p + 2 * x
        return jnp.where(
            lane < 2,
            pltpu.roll(east_ref[block], (-at) % LANE, 1),
            jnp.where(lane >= LANE - 2, pltpu.roll(west_ref[block], (LANE - 2 - at) % LANE, 1), 0.0),
        )

    for x in range(rows + 4):
        for c in range(3):
            now_x[c, x, :, :LANE] = plane_row(refs, lev, rows, c, x)
            now_x[c, x, :, LANE:] = sides(c, x)
        for k in range(2):
            mods_ref[k, x, :, :LANE] = plane_row(refs, lev, rows, 3 + k, x)
            mods_ref[k, x, :, LANE:] = sides(3 + k, x)
        if 1 <= x < rows + 3:
            for c in range(3):
                base_ref[c, x, :, :LANE] = plane_row(refs, lev, rows, 5 + c, x)
                base_ref[c, x, :, LANE:] = sides(5 + c, x)
            for part, v in ((slice(0, LANE), plane_row(refs, lev, rows, 8, x)), (slice(LANE, WIDE), sides(8, x))):
                there = v > 0.0
                scale_ref[x, :, part] = jnp.where(there, step_square / jnp.where(there, v, 1.0), 0.0)

    def first(x):
        quarter_row(mods_ref, coef, x)
        parts = east_flow([now_x[c, x] for c in range(3)], coef, x)
        for i in range(3):
            flow[i, x] = parts[i]

    rows_loop(0, rows + 4, 10, first)
    rows_loop(1, rows + 3, 6, lambda x: coef_row(mods_ref, coef, x))

    def second(x):
        applied = apply_row(lambda c, r: now_x[c, r], lambda i, r: flow[i, r], coef, x, WIDE)
        for c in range(3):
            base_ref[c, x] = 2.0 * now_x[c, x] - base_ref[c, x] + scale_ref[x] * applied[c]

    rows_loop(1, rows + 3, 9, second)

    group_of_sub = sub // 2
    second_level = (sub - 2 * group_of_sub).astype(jnp.float32)
    k_row = sub_ids((LANE, LANE))
    k_lane = lane_ids((LANE, LANE))
    sub_f = sub.astype(jnp.float32)
    for t in range(3):
        def entry(column, i):
            return metas[column][t : t + 1, i : i + 1]

        for column in range(3):
            low = entry(column, 3 * groups)
            high = entry(column, 3 * groups + 1)
            outer = (sub_f < low).astype(jnp.float32)
            inner = ((sub_f >= low) & (sub_f < high)).astype(jnp.float32)
            if column == 0:
                mask_ref[0, t, :, :LANE] = outer
                mask_ref[1, t, :, :LANE] = inner
            elif column == 1:
                east_masks = (outer, inner)
            else:
                for q, own in enumerate((outer, inner)):
                    mask_ref[q, t, :, LANE:] = jnp.where(lane < LANE // 2, east_masks[q], own)
            depth = second_level
            east_at = jnp.zeros((lev, LANE), jnp.float32)
            hold = jnp.zeros((lev, LANE), jnp.float32)
            north_at = jnp.zeros((LANE, LANE), jnp.float32)
            point = jnp.zeros((LANE, LANE), jnp.float32)
            for g in range(groups):
                here = group_of_sub == g
                depth = jnp.where(here, second_level + entry(column, 3 * g), depth)
                east_at = jnp.where(here, 4.0 * entry(column, 3 * g + 1), east_at)
                mine = here & (lane >= g * c_north) & (lane < (g + 1) * c_north)
                hold = jnp.where(mine & (high > 2.0 * g + 1.0), 1.0 / 625.0, hold)
                there = (k_row >= g * c_north) & (k_row < (g + 1) * c_north)
                north_at = jnp.where(there, 4.0 * entry(column, 3 * g + 2), north_at)
                point = jnp.where(there, 25.0 * (k_row - g * c_north).astype(jnp.float32), point)
            depth = depth * (4.0 / 25.0)
            level_ref[t, column, 0] = hold * (1.0 - depth)
            level_ref[t, column, 1] = hold * depth
            hat = jnp.maximum(25.0 - jnp.abs(north_at + 4.0 * k_lane.astype(jnp.float32) - point), 0.0)
            hat = jnp.where(k_row < groups * c_north, hat, 0.0)
            if column == 0:
                shift_ref[t, :, :LANE] = east_at
                own_hat_ref[t] = hat.astype(jnp.bfloat16)
            elif column == 1:
                east_shift = east_at
                side_hat_ref[t, :LANE, :] = jnp.where(k_lane < LANE // 2, hat, 0.0).astype(jnp.bfloat16)
            else:
                shift_ref[t, :, LANE:] = jnp.where(lane < LANE // 2, east_shift, east_at)
                side_hat_ref[t, LANE:, :] = jnp.where(k_lane >= LANE // 2, hat, 0.0).astype(jnp.bfloat16)


def split_dot(ref, hat):
    v = ref[...]
    high = v.astype(jnp.bfloat16)
    low = (v - high.astype(jnp.float32)).astype(jnp.bfloat16)
    return jnp.dot(high, hat, preferred_element_type=jnp.float32) + jnp.dot(
        low, hat, preferred_element_type=jnp.float32
    )


def finish_kernel(
    lev, rows, groups, c_east, c_north, got_ref, index_ref, mods_ref, base_ref, scale_ref, mask_ref,
    level_ref, shift_ref, own_hat_ref, side_hat_ref, now_ref, inc_out, mid_out, next_out,
    mixed, own_rows, side_rows, north, parts, flow, mid, coef
):
    lane = lane_ids((8, LANE))
    rows_loop(0, rows + 4, 5, lambda x: quarter_row(mods_ref, coef, x))
    rows_loop(1, rows + 3, 6, lambda x: coef_row(mods_ref, coef, x))

    def tile_row(t, carry):
        for column in range(3):
            pieces = []
            for g in range(groups):
                b = index_ref[(t * 3 + column) * groups + g]
                source = b >> 1
                k = b & 1
                top = pl.multiple_of(8 * k, 8)
                third = got_ref[source, 24:32, :]
                fourth = got_ref[source, 32:40, :]
                tail = jnp.where(lane < 40, pltpu.roll(third, LANE - 80, 1), pltpu.roll(fourth, LANE - 40, 1))
                pieces.append(
                    (
                        (got_ref[source, pl.ds(top, 8), :], got_ref[source, pl.ds(24 + top, 8), :]),
                        (pltpu.roll(got_ref[source, 16:24, :], 4 * k, 0), pltpu.roll(tail, 4 * k, 0)),
                    )
                )
            for a in range(c_east):
                start = a * c_north
                for half in range(2):
                    total = jnp.zeros((8, LANE), jnp.float32)
                    for g in range(groups):
                        body, tail = pieces[g][half]
                        at = g * c_north
                        if start + c_north <= LANE:
                            moved = pltpu.roll(body, (at - start) % LANE, 1)
                        elif start >= LANE:
                            moved = pltpu.roll(tail, (at - start) % LANE, 1)
                        else:
                            moved = jnp.where(
                                lane < at + LANE - start,
                                pltpu.roll(body, (at - start) % LANE, 1),
                                pltpu.roll(tail, (at - start) % LANE, 1),
                            )
                        total = jnp.where((lane >= at) & (lane < at + c_north), moved, total)
                    mixed[a, 8 * half : 8 * half + 8, :] = total
            w0 = level_ref[t, column, 0]
            w1 = level_ref[t, column, 1]
            for nc in range(6):
                r = (nc // 3) * 6 + 2 * (nc % 3)
                for a in range(c_east):
                    value = w0 * jnp.broadcast_to(mixed[a, r : r + 1, :], (lev, LANE)) + w1 * jnp.broadcast_to(
                        mixed[a, r + 1 : r + 2, :], (lev, LANE)
                    )
                    at = (nc * c_east + a) * lev
                    if column == 0:
                        own_rows[at : at + lev, :] = value
                    elif column == 1:
                        side_rows[at : at + lev, :LANE] = value
                    else:
                        side_rows[at : at + lev, LANE:] = value
        own = split_dot(own_rows, own_hat_ref[t])
        north[t, :, :, :LANE] = own.reshape(6 * c_east, lev, LANE)
        side = split_dot(side_rows, side_hat_ref[t])
        north[t, :, :, LANE:] = side.reshape(6 * c_east, lev, LANE)
        return carry

    lax.fori_loop(0, 3, tile_row, 0)

    near = (4 * 24) // 25 + 3

    def east(x, t, cell):
        first = 4 * cell // 25 if isinstance(cell, int) else lax.div(4 * cell, 25)
        ahead = 4 * cell - 25 * first
        at = shift_ref[t] + (float(ahead) if isinstance(cell, int) else ahead.astype(jnp.float32))
        weights = [jnp.maximum(25.0 - jnp.abs(at - 25.0 * i), 0.0) for i in range(near)]
        outer = mask_ref[0, t]
        inner = mask_ref[1, t]
        values = []
        for nc in range(6):
            total = None
            for i in range(near):
                term = weights[i] * north[t, nc * c_east + first + i]
                total = term if total is None else total + term
            values.append(total)
            parts[nc, x] = outer * total
            parts[6 + nc, x] = inner * total
            if not isinstance(cell, int):
                inc_out[pl.ds(nc * lev * rows + cell, lev, stride=rows), :] = total[:, :LANE]
        for n in range(2):
            for q, mask in enumerate((outer, inner)):
                moved = east_flow([mask * values[3 * n + c] for c in range(3)], coef, x)
                for i in range(3):
                    flow[6 * n + 3 * q + i, x] = moved[i]

    rows_loop(0, rows, 8, lambda cell: east(cell + 2, 1, cell))
    for r in range(2):
        east(r, 0, rows - 2 + r)
        east(rows + 2 + r, 2, r)

    def forcing(step, x, t, width):
        outside = apply_row(
            lambda c, r: parts[3 * step + c, r], lambda i, r: flow[6 * step + i, r], coef, x, width
        )
        inside = apply_row(
            lambda c, r: parts[6 + 3 * step + c, r], lambda i, r: flow[6 * step + 3 + i, r], coef, x, width
        )
        outer = mask_ref[0, t][:, :width]
        inner = mask_ref[1, t][:, :width]
        return [inner * outside[c] - outer * inside[c] for c in range(3)]

    def middle(x):
        t = (x >= 2).astype(jnp.int32) + (x >= rows + 2).astype(jnp.int32)
        force = forcing(0, x, t, WIDE)
        for c in range(3):
            mid[c, x] = base_ref[c, x] + scale_ref[x] * force[c]

    rows_loop(1, rows + 3, 9, middle)

    def flows(x):
        moved = east_flow([mid[c, x] for c in range(3)], coef, x)
        for i in range(3):
            flow[12 + i, x] = moved[i]

    rows_loop(1, rows + 3, 18, flows)

    def last(x):
        force = forcing(1, x, 1, LANE)
        applied = apply_row(lambda c, r: mid[c, r], lambda i, r: flow[12 + i, r], coef, x, LANE)
        scale = scale_ref[x, :, :LANE]
        for c in range(3):
            now = now_ref[pl.ds(c * lev * rows + x - 2, lev, stride=rows), :]
            current = mid[c, x, :, :LANE]
            mid_out[pl.ds(c * lev * rows + x - 2, lev, stride=rows), :] = current
            next_out[pl.ds(c * lev * rows + x - 2, lev, stride=rows), :] = (
                2.0 * current - now + scale * (applied[c] + force[c])
            )

    rows_loop(2, rows + 2, 16, last)


def specs(text):
    space = {"v": VMEM, "s": SMEM, "h": pltpu.HBM}
    return [pl.BlockSpec(memory_space=space[kind]) for kind in text]


def f32(*shape):
    return jax.ShapeDtypeStruct(shape, jnp.float32)


def neighbours(axis, step):
    count = lax.axis_size(axis)
    return [(i, i + step) for i in range(count) if 0 <= i + step < count]


def local(disp_now, disp_prev, density, moduli, coarse, block_route, ranges, offsets):
    _, lev, rows, north_cells = disp_now.shape
    groups = lev // 2
    c_east = (rows + 23) * 4 // 25 + 2
    c_north = (north_cells + 23) * 4 // 25 + 2
    block_hold = coarse.shape[0]
    samples = coarse.shape[1] // 6
    n_x = lax.axis_size("gx")
    n_y = lax.axis_size("gy")
    assert lev == 8 and north_cells == LANE and block_hold == 2
    assert (c_east, c_north) == (8, 26) and 6 * (rows + 4) <= LANE
    now, prev, dens, mods = (a.reshape(-1, north_cells) for a in (disp_now, disp_prev, density, moduli))
    wide = rows + 4
    shifts = offsets.transpose(0, 3, 1, 2)
    limit = pltpu.CompilerParams(vmem_limit_bytes=16 * 2**20)
    assert n_x % 2 == 0

    payload, first, last = pl.pallas_call(
        functools.partial(pre_kernel, lev, rows, groups, samples),
        out_shape=(f32(40, LANE), f32(15, lev, LANE), f32(15, lev, LANE)),
        in_specs=specs("hhhhhss"),
        out_specs=specs("vvv"),
        scratch_shapes=[VMEM((24, WIDE), jnp.float32)]
        + [VMEM(a.shape, jnp.float32) for a in (coarse, now, prev, dens, mods)]
        + [pltpu.SemaphoreType.DMA((5,))],
        compiler_params=limit,
        name="pre",
    )(*(pltpu.with_memory_space_constraint(a, pltpu.HBM) for a in (coarse, now, prev, dens, mods, shifts, ranges)))
    half = n_x * n_y // 2
    twin = lax.ppermute(payload, "gx", [(i, (i + n_x // 2) % n_x) for i in range(n_x)])
    before = lax.ppermute(last, "gx", neighbours("gx", 1))
    after = lax.ppermute(first, "gx", neighbours("gx", -1))
    chunk = jnp.concatenate([payload, twin], axis=0)
    got = lax.all_to_all(
        jnp.broadcast_to(chunk[None], (half,) + chunk.shape),
        ("gx", "gy"),
        split_axis=0,
        concat_axis=0,
        tiled=True,
        axis_index_groups=[list(range(half)), list(range(half, 2 * half))],
    ).reshape(2 * half, 40, LANE)
    to_west, to_east, meta = pl.pallas_call(
        functools.partial(pack_kernel, lev, rows),
        out_shape=(f32(4, lev, LANE), f32(4, lev, LANE), f32(lev, LANE)),
        in_specs=specs("vvvvvvv"),
        out_specs=specs("vvv"),
        cost_estimate=pl.CostEstimate(flops=2000000, bytes_accessed=1000000, transcendentals=0),
        compiler_params=limit,
        name="pack",
    )(now, prev, dens, mods, before, after, first)
    west = lax.ppermute(to_east, "gy", neighbours("gy", 1))
    east = lax.ppermute(to_west, "gy", neighbours("gy", -1))
    place = jnp.stack([lax.axis_index("gx"), lax.axis_index("gy")]).astype(jnp.int32)
    index = pl.pallas_call(
        functools.partial(index_kernel, groups, n_x, n_y),
        out_shape=jax.ShapeDtypeStruct((9 * groups + 1,), jnp.int32),
        in_specs=specs("ss"),
        out_specs=specs("s")[0],
        compiler_params=limit,
        cost_estimate=pl.CostEstimate(flops=2000000, bytes_accessed=1000, transcendentals=0),
        name="index",
    )(block_route, place)
    prepared = pl.pallas_call(
        functools.partial(prep_kernel, lev, rows, groups, c_north),
        out_shape=(
            f32(2, wide, lev, WIDE),
            f32(3, wide, lev, WIDE),
            f32(wide, lev, WIDE),
            f32(2, 3, lev, WIDE),
            f32(3, 3, 2, lev, LANE),
            f32(3, lev, WIDE),
            jax.ShapeDtypeStruct((3, LANE, LANE), jnp.bfloat16),
            jax.ShapeDtypeStruct((3, WIDE, LANE), jnp.bfloat16),
        ),
        in_specs=specs("v" * 9),
        out_specs=specs("v" * 8),
        scratch_shapes=[
            VMEM((3, wide, lev, WIDE), jnp.float32),
            VMEM((3, wide, lev, WIDE), jnp.float32),
            VMEM((COEFS, wide, lev, WIDE), jnp.float32),
        ],
        cost_estimate=pl.CostEstimate(flops=10000000, bytes_accessed=3000000, transcendentals=0),
        compiler_params=limit,
        name="prep",
    )(now, prev, dens, mods, before, after, west, east, meta)
    mods_x, base, scale, mask, level_w, shift, own_hat, side_hat = prepared
    incident, mid, nxt = pl.pallas_call(
        functools.partial(finish_kernel, lev, rows, groups, c_east, c_north),
        out_shape=(
            f32(6 * lev * rows, LANE),
            f32(3 * lev * rows, LANE),
            f32(3 * lev * rows, LANE),
        ),
        in_specs=specs("vsvvvvvvvvv"),
        out_specs=specs("vvv"),
        scratch_shapes=[
            VMEM((c_east, 16, LANE), jnp.float32),
            VMEM((6 * c_east * lev, LANE), jnp.float32),
            VMEM((6 * c_east * lev, WIDE), jnp.float32),
            VMEM((3, 6 * c_east, lev, WIDE), jnp.float32),
            VMEM((12, wide, lev, WIDE), jnp.float32),
            VMEM((15, wide, lev, WIDE), jnp.float32),
            VMEM((3, wide, lev, WIDE), jnp.float32),
            VMEM((COEFS, wide, lev, WIDE), jnp.float32),
        ],
        cost_estimate=pl.CostEstimate(flops=20000000, bytes_accessed=6000000, transcendentals=0),
        compiler_params=limit,
        name="finish",
    )(got, index, mods_x, base, scale, mask, level_w, shift, own_hat, side_hat, now)
    return (
        incident.reshape(2, 3, lev, rows, north_cells),
        mid.reshape(disp_now.shape),
        nxt.reshape(disp_now.shape),
    )


def solution(mesh):
    return jax.shard_map(
        local,
        mesh=mesh,
        in_specs=(
            P(None, None, "gx", "gy"),
            P(None, None, "gx", "gy"),
            P(None, "gx", "gy"),
            P(None, None, "gx", "gy"),
            P(("gx", "gy"), None, None),
            P(),
            P("gx", "gy", None),
            P("gx", "gy", None, None),
        ),
        out_specs=(
            P(None, None, None, "gx", "gy"),
            P(None, None, "gx", "gy"),
            P(None, None, "gx", "gy"),
        ),
        check_vma=False,
    )
```

```python
import functools

import jax
import jax.numpy as jnp
from jax import lax
from jax.experimental import pallas as pl
from jax.experimental.pallas import tpu as pltpu
from jax.sharding import PartitionSpec as P


step_square = 0.05
time_weights = ((-0.0595, 0.7735, 0.3315, -0.0455), (-0.063756, 0.607068, 0.517132, -0.060444))

LANE = 128
WIDE = 256
VMEM = pltpu.VMEM
SMEM = pltpu.SMEM


def lane_ids(shape):
    return lax.broadcasted_iota(jnp.int32, shape, len(shape) - 1)


def sub_ids(shape):
    return lax.broadcasted_iota(jnp.int32, shape, len(shape) - 2)


def shift_up(u):
    count = u.shape[0]
    return jnp.where(sub_ids(u.shape) == count - 1, 0.0, pltpu.roll(u, count - 1, 0))


def shift_down(u):
    return jnp.where(sub_ids(u.shape) == 0, 0.0, pltpu.roll(u, 1, 0))


def shift_next(u):
    return pltpu.roll(u, u.shape[1] - 1, 1)


def shift_prior(u):
    return pltpu.roll(u, 1, 1)


def level_row(ref, plane, levels, rows, r):
    return ref[pl.ds(plane * levels * rows + r, levels, stride=rows), :]


def rows_loop(start, stop, most, body):
    step = max(d for d in range(1, most + 1) if (stop - start) % d == 0)

    if step == stop - start:
        for x in range(start, stop):
            body(x)
        return

    def chunk(i, carry):
        for r in range(step):
            body(start + i * step + r)
        return carry

    lax.fori_loop(0, (stop - start) // step, chunk, 0)


def quotient(v, n):
    return v >> (n.bit_length() - 1) if n & (n - 1) == 0 else lax.div(v, n)


def meta_vector(off_ref, rng_ref, groups):
    shape = (8, LANE)
    lane = lane_ids(shape)
    out = jnp.zeros(shape, jnp.float32)
    for g in range(groups):
        for q in range(3):
            out = jnp.where(lane == 3 * g + q, off_ref[0, q, 0, g].astype(jnp.float32), out)
    for q in range(2):
        out = jnp.where(lane == 3 * groups + q, rng_ref[0, 0, q].astype(jnp.float32), out)
    return out


def pre_kernel(
    lev, rows, groups, samples, *refs
):
    sources, (off_ref, rng_ref, pay_ref, first_ref, last_ref, scr) = refs[:5], refs[5:11]
    held, sems = refs[11:16], refs[16]
    copies = [pltpu.make_async_copy(sources[i], held[i], sems.at[i]) for i in range(5)]
    for copy in copies:
        copy.start()
    coarse_ref, now_ref, prev_ref, dens_ref, mod_ref = held
    copies[0].wait()
    for k in range(coarse_ref.shape[0]):
        mixed = []
        for n in range(2):
            total = None
            for t in range(samples):
                term = time_weights[n][t] * coarse_ref[k, 6 * t : 6 * t + 6, :]
                total = term if total is None else total + term
            mixed.append(total)
        scr[8 * k : 8 * k + 6, :] = mixed[0]
        scr[8 * k + 6 : 8 * k + 8, :] = mixed[1][0:2]
        scr[16 + 4 * k : 20 + 4 * k, :] = mixed[1][2:6]
    head = [scr[8 * i : 8 * i + 8, :LANE] for i in range(3)]
    tail = [scr[8 * i : 8 * i + 8, LANE:] for i in range(3)]
    lane = lane_ids((8, LANE))
    tiles = head + [
        jnp.where(lane < 80, tail[0], pltpu.roll(tail[2], 80, 1)),
        jnp.where(lane < 80, tail[1], pltpu.roll(tail[2], 40, 1)),
    ]

    for i, tile in enumerate(tiles):
        pay_ref[8 * i : 8 * i + 8, :] = tile
    meta = meta_vector(off_ref, rng_ref, groups)
    for copy in copies[1:]:
        copy.wait()
    for ref, start, edge in ((first_ref, 0, 0), (last_ref, rows - 2, rows - 1)):
        for c in range(3):
            for r in range(2):
                ref[2 * c + r] = level_row(now_ref, c, lev, rows, start + r)
            ref[10 + c] = level_row(prev_ref, c, lev, rows, edge)
        for k in range(2):
            for r in range(2):
                ref[6 + 2 * k + r] = level_row(mod_ref, k, lev, rows, start + r)
        ref[13] = level_row(dens_ref, 0, lev, rows, edge)
        ref[14] = meta


def plane_row(refs, lev, rows, plane, x):
    now_ref, prev_ref, dens_ref, mod_ref, before_ref, after_ref = refs
    if plane < 3:
        source, own, strip, both = now_ref, plane, 2 * plane, True
    elif plane < 5:
        source, own, strip, both = mod_ref, plane - 3, 6 + 2 * (plane - 3), True
    elif plane < 8:
        source, own, strip, both = prev_ref, plane - 5, 10 + plane - 5, False
    else:
        source, own, strip, both = dens_ref, 0, 13, False
    if 2 <= x < rows + 2:
        return level_row(source, own, lev, rows, x - 2)
    ref, r = (before_ref, x) if x < 2 else (after_ref, x - rows - 2)
    if both:
        return ref[strip + r]
    return ref[strip] if x in (1, rows + 2) else None


def pack_kernel(
    lev, rows, now_ref, prev_ref, dens_ref, mod_ref, before_ref, after_ref, own_ref,
    west_ref, east_ref, meta_ref
):
    refs = (now_ref, prev_ref, dens_ref, mod_ref, before_ref, after_ref)
    lane = lane_ids((lev, LANE))
    span = 2 * (rows + 4)
    for block in range(3):
        west = jnp.zeros((lev, LANE), jnp.float32)
        east = jnp.zeros((lev, LANE), jnp.float32)
        for p in range(3):
            for x in range(rows + 4):
                v = plane_row(refs, lev, rows, 3 * block + p, x)
                if v is None:
                    continue
                at = span * p + 2 * x
                here = (lane == at) | (lane == at + 1)
                west = jnp.where(here, pltpu.roll(v, at, 1), west)
                east = jnp.where(here, pltpu.roll(v, (at + 2) % LANE, 1), east)
        west_ref[block] = west
        east_ref[block] = east
    sub = sub_ids((lev, LANE))
    both = jnp.where(sub == 0, before_ref[14], jnp.where(sub == 1, own_ref[14], after_ref[14]))
    west_ref[3] = both
    east_ref[3] = both
    meta_ref[...] = both


MU = {"l+": 0, "l-": 1, "e+": 2, "e-": 3, "n+": 4, "n-": 5}
STIFF = {"l+": 6, "l-": 7, "e+": 8, "e-": 9, "n+": 10, "n-": 11}
CENTER = 12
MU_QUARTER = 15
LAME_QUARTER = 16
COEFS = 17


def quarter_row(mod_ref, coef_ref, x):
    coef_ref[MU_QUARTER, x] = 0.25 * mod_ref[0, x]
    coef_ref[LAME_QUARTER, x] = 0.25 * mod_ref[1, x]


def coef_row(mod_ref, coef_ref, x):
    sums = []
    for stiff, table in ((False, MU), (True, STIFF)):

        def half(r):
            mu = mod_ref[0, r]
            return 0.5 * mod_ref[1, r] + mu if stiff else 0.5 * mu

        k = half(x)
        values = {
            "l+": k + shift_up(k),
            "l-": k + shift_down(k),
            "e+": k + half(x + 1),
            "e-": k + half(x - 1),
            "n+": k + shift_next(k),
            "n-": k + shift_prior(k),
        }
        for name, value in values.items():
            coef_ref[table[name], x] = value
        sums.append({d: values[d + "+"] + values[d + "-"] for d in "len"})
    soft, hard = sums
    coef_ref[CENTER + 0, x] = hard["l"] + soft["e"] + soft["n"]
    coef_ref[CENTER + 1, x] = soft["l"] + hard["e"] + soft["n"]
    coef_ref[CENTER + 2, x] = soft["l"] + soft["e"] + hard["n"]


def east_flow(u, coef_ref, x):
    mu = coef_ref[MU_QUARTER, x]
    lame = coef_ref[LAME_QUARTER, x]
    rise = [shift_up(u[c]) - shift_down(u[c]) for c in range(2)]
    run = [shift_next(u[c]) - shift_prior(u[c]) for c in (1, 2)]
    return mu * rise[1], lame * (rise[0] + run[1]), mu * run[0]


def apply_row(field, flow, coef_ref, x, width):
    def cut(v):
        return v[:, :width]

    u = [field(c, x) for c in range(3)]
    after = [field(c, x + 1) for c in range(3)]
    before = [field(c, x - 1) for c in range(3)]
    up = [shift_up(v) for v in u]
    down = [shift_down(v) for v in u]
    nxt = [shift_next(v) for v in u]
    prior = [shift_prior(v) for v in u]
    d_l = [up[c] - down[c] for c in range(3)]
    d_n = [nxt[c] - prior[c] for c in range(3)]
    d_e = [after[c] - before[c] for c in range(3)]
    mu = coef_ref[MU_QUARTER, x]
    lame = coef_ref[LAME_QUARTER, x]
    level_flow = (cut(lame * (d_e[1] + d_n[2])), cut(mu * d_e[0]), cut(mu * d_n[0]))
    north_flow = (mu * d_l[2], mu * d_e[2], lame * (d_l[0] + d_e[1]))
    out = []
    for i in range(3):

        def coef(name):
            table = STIFF if "len".index(name[0]) == i else MU
            return cut(coef_ref[table[name], x])

        total = cut(flow(i, x + 1)) - cut(flow(i, x - 1))
        total += shift_up(level_flow[i]) - shift_down(level_flow[i])
        total += cut(shift_next(north_flow[i]) - shift_prior(north_flow[i]))
        total += coef("l+") * cut(up[i]) + coef("l-") * cut(down[i])
        total += coef("e+") * cut(after[i]) + coef("e-") * cut(before[i])
        total += coef("n+") * cut(nxt[i]) + coef("n-") * cut(prior[i])
        total -= cut(coef_ref[CENTER + i, x]) * cut(u[i])
        out.append(total)
    return out


def index_kernel(groups, n_x, n_y, route_ref, place_ref, index_ref):
    my_x, my_y = place_ref[0], place_ref[1]
    for i in range(9 * groups):
        index_ref[i] = 0
    half = n_x * n_y // 2
    upper = (2 * my_x >= n_x).astype(jnp.int32)

    def find(b):
        slot = route_ref[b]
        tile = quotient(slot, groups)
        tile_x = quotient(tile, n_y)
        d_x = tile_x - my_x + 1
        d_y = tile - tile_x * n_y - my_y
        column = jnp.where(d_y < 0, 2, d_y)
        near = (d_x >= 0) & (d_x < 3) & (d_y >= -1) & (d_y < 2)
        at = jnp.where(near, (d_x * 3 + column) * groups + slot - tile * groups, 9 * groups)
        source = quotient(b, 2)
        far = (source >= half).astype(jnp.int32)
        seat = 2 * (source - far * half) + (far ^ upper)
        index_ref[at] = 2 * seat + b - 2 * source

    rows_loop(0, route_ref.shape[0], 16, find)


def prep_kernel(
    lev, rows, groups, c_north, now_ref, prev_ref, dens_ref, mod_ref, before_ref, after_ref, west_ref, east_ref, meta_ref,
    mods_ref, base_ref, scale_ref, mask_ref, level_ref, shift_ref, own_hat_ref, side_hat_ref,
    now_x, flow, coef
):
    refs = (now_ref, prev_ref, dens_ref, mod_ref, before_ref, after_ref)
    lane = lane_ids((lev, LANE))
    sub = sub_ids((lev, LANE))
    span = 2 * (rows + 4)

    metas = (meta_ref[...], east_ref[3], west_ref[3])

    def sides(plane, x):
        block, p = divmod(plane, 3)
        at = span * p + 2 * x
        return jnp.where(
            lane < 2,
            pltpu.roll(east_ref[block], (-at) % LANE, 1),
            jnp.where(lane >= LANE - 2, pltpu.roll(west_ref[block], (LANE - 2 - at) % LANE, 1), 0.0),
        )

    for x in range(rows + 4):
        for c in range(3):
            now_x[c, x, :, :LANE] = plane_row(refs, lev, rows, c, x)
            now_x[c, x, :, LANE:] = sides(c, x)
        for k in range(2):
            mods_ref[k, x, :, :LANE] = plane_row(refs, lev, rows, 3 + k, x)
            mods_ref[k, x, :, LANE:] = sides(3 + k, x)
        if 1 <= x < rows + 3:
            for c in range(3):
                base_ref[c, x, :, :LANE] = plane_row(refs, lev, rows, 5 + c, x)
                base_ref[c, x, :, LANE:] = sides(5 + c, x)
            for part, v in ((slice(0, LANE), plane_row(refs, lev, rows, 8, x)), (slice(LANE, WIDE), sides(8, x))):
                there = v > 0.0
                scale_ref[x, :, part] = jnp.where(there, step_square / jnp.where(there, v, 1.0), 0.0)

    def first(x):
        quarter_row(mods_ref, coef, x)
        parts = east_flow([now_x[c, x] for c in range(3)], coef, x)
        for i in range(3):
            flow[i, x] = parts[i]

    rows_loop(0, rows + 4, rows + 4, first)
    rows_loop(1, rows + 3, rows + 2, lambda x: coef_row(mods_ref, coef, x))

    def second(x):
        applied = apply_row(lambda c, r: now_x[c, r], lambda i, r: flow[i, r], coef, x, WIDE)
        for c in range(3):
            base_ref[c, x] = 2.0 * now_x[c, x] - base_ref[c, x] + scale_ref[x] * applied[c]

    rows_loop(1, rows + 3, rows + 2, second)

    group_of_sub = sub // 2
    second_level = (sub - 2 * group_of_sub).astype(jnp.float32)
    k_row = sub_ids((LANE, LANE))
    k_lane = lane_ids((LANE, LANE))
    sub_f = sub.astype(jnp.float32)
    for t in range(3):
        def entry(column, i):
            return metas[column][t : t + 1, i : i + 1]

        for column in range(3):
            low = entry(column, 3 * groups)
            high = entry(column, 3 * groups + 1)
            outer = (sub_f < low).astype(jnp.float32)
            inner = ((sub_f >= low) & (sub_f < high)).astype(jnp.float32)
            if column == 0:
                mask_ref[0, t, :, :LANE] = outer
                mask_ref[1, t, :, :LANE] = inner
            elif column == 1:
                east_masks = (outer, inner)
            else:
                for q, own in enumerate((outer, inner)):
                    mask_ref[q, t, :, LANE:] = jnp.where(lane < LANE // 2, east_masks[q], own)
            depth = second_level
            east_at = jnp.zeros((lev, LANE), jnp.float32)
            hold = jnp.zeros((lev, LANE), jnp.float32)
            north_at = jnp.zeros((LANE, LANE), jnp.float32)
            point = jnp.zeros((LANE, LANE), jnp.float32)
            for g in range(groups):
                here = group_of_sub == g
                depth = jnp.where(here, second_level + entry(column, 3 * g), depth)
                east_at = jnp.where(here, 4.0 * entry(column, 3 * g + 1), east_at)
                mine = here & (lane >= g * c_north) & (lane < (g + 1) * c_north)
                hold = jnp.where(mine & (high > 2.0 * g + 1.0), 1.0 / 625.0, hold)
                there = (k_row >= g * c_north) & (k_row < (g + 1) * c_north)
                north_at = jnp.where(there, 4.0 * entry(column, 3 * g + 2), north_at)
                point = jnp.where(there, 25.0 * (k_row - g * c_north).astype(jnp.float32), point)
            depth = depth * (4.0 / 25.0)
            level_ref[t, column, 0] = hold * (1.0 - depth)
            level_ref[t, column, 1] = hold * depth
            hat = jnp.maximum(25.0 - jnp.abs(north_at + 4.0 * k_lane.astype(jnp.float32) - point), 0.0)
            hat = jnp.where(k_row < groups * c_north, hat, 0.0)
            if column == 0:
                shift_ref[t, :, :LANE] = east_at
                own_hat_ref[t] = hat.astype(jnp.bfloat16)
            elif column == 1:
                east_shift = east_at
                side_hat_ref[t, :LANE, :] = jnp.where(k_lane < LANE // 2, hat, 0.0).astype(jnp.bfloat16)
            else:
                shift_ref[t, :, LANE:] = jnp.where(lane < LANE // 2, east_shift, east_at)
                side_hat_ref[t, LANE:, :] = jnp.where(k_lane >= LANE // 2, hat, 0.0).astype(jnp.bfloat16)


def split_dot(v, hat):
    high = v.astype(jnp.bfloat16)
    low = (v - high.astype(jnp.float32)).astype(jnp.bfloat16)
    if v.shape[1] == LANE:
        both = jnp.concatenate([high, low], axis=1)
        return jnp.dot(both, jnp.concatenate([hat, hat], axis=0), preferred_element_type=jnp.float32)
    return jnp.dot(high, hat, preferred_element_type=jnp.float32) + jnp.dot(
        low, hat, preferred_element_type=jnp.float32
    )


def finish_kernel(
    lev, rows, groups, c_east, c_north, got_ref, index_ref, mods_ref, base_ref, scale_ref, mask_ref,
    level_ref, shift_ref, own_hat_ref, side_hat_ref, now_ref, inc_out, mid_out, next_out,
    mixed, own_rows, side_rows, north, parts, flow, mid, coef, inc_held, mid_held, next_held, sems
):
    lane = lane_ids((8, LANE))
    outs = ((inc_held, inc_out), (mid_held, mid_out), (next_held, next_out))
    rows_loop(0, rows + 4, rows + 4, lambda x: quarter_row(mods_ref, coef, x))
    rows_loop(1, rows + 3, rows + 2, lambda x: coef_row(mods_ref, coef, x))

    def tile_row(t):
        cells = range(rows) if t == 1 else range(rows - 2, rows) if t == 0 else range(2)
        used = range(4 * cells[0] // 25, (4 * (cells[-1] + 24)) // 25 + 2)
        for column in range(3):
            pieces = []
            for g in range(groups):
                b = index_ref[(t * 3 + column) * groups + g]
                source = b >> 1
                k = b & 1
                top = pl.multiple_of(8 * k, 8)
                third = got_ref[source, 24:32, :]
                fourth = got_ref[source, 32:40, :]
                tail = jnp.where(lane < 40, pltpu.roll(third, LANE - 80, 1), pltpu.roll(fourth, LANE - 40, 1))
                pieces.append(
                    (
                        (got_ref[source, pl.ds(top, 8), :], got_ref[source, pl.ds(24 + top, 8), :]),
                        (pltpu.roll(got_ref[source, 16:24, :], 4 * k, 0), pltpu.roll(tail, 4 * k, 0)),
                    )
                )
            for a in used:
                start = a * c_north
                for half in range(2):
                    total = jnp.zeros((8, LANE), jnp.float32)
                    for g in range(groups):
                        body, tail = pieces[g][half]
                        at = g * c_north
                        if start + c_north <= LANE:
                            moved = pltpu.roll(body, (at - start) % LANE, 1)
                        elif start >= LANE:
                            moved = pltpu.roll(tail, (at - start) % LANE, 1)
                        else:
                            moved = jnp.where(
                                lane < at + LANE - start,
                                pltpu.roll(body, (at - start) % LANE, 1),
                                pltpu.roll(tail, (at - start) % LANE, 1),
                            )
                        total = jnp.where((lane >= at) & (lane < at + c_north), moved, total)
                    mixed[t, column, a, 8 * half : 8 * half + 8, :] = total
            w0 = level_ref[t, column, 0]
            w1 = level_ref[t, column, 1]
            for nc in range(6):
                r = (nc // 3) * 6 + 2 * (nc % 3)
                for a in used:
                    value = w0 * jnp.broadcast_to(mixed[t, column, a, r : r + 1, :], (lev, LANE)) + w1 * jnp.broadcast_to(
                        mixed[t, column, a, r + 1 : r + 2, :], (lev, LANE)
                    )
                    at = (nc * len(used) + a - used[0]) * lev
                    if column == 0:
                        own_rows[t, at : at + lev, :] = value
                    elif column == 1:
                        side_rows[t, at : at + lev, :LANE] = value
                    else:
                        side_rows[t, at : at + lev, LANE:] = value
        count = 6 * len(used) * lev
        own = split_dot(own_rows[t, :count, :], own_hat_ref[t])
        side = split_dot(side_rows[t, :count, :], side_hat_ref[t])
        for nc in range(6):
            part = slice(nc * len(used) * lev, (nc + 1) * len(used) * lev)
            to = slice(nc * c_east + used[0], nc * c_east + used[-1] + 1)
            north[t, to, :, :LANE] = own[part].reshape(len(used), lev, LANE)
            north[t, to, :, LANE:] = side[part].reshape(len(used), lev, LANE)

    for t in range(3):
        tile_row(t)

    near = (4 * 24) // 25 + 3

    def east(x, t, cell):
        first = 4 * cell // 25 if isinstance(cell, int) else lax.div(4 * cell, 25)
        ahead = 4 * cell - 25 * first
        at = shift_ref[t] + (float(ahead) if isinstance(cell, int) else ahead.astype(jnp.float32))
        weights = [jnp.maximum(25.0 - jnp.abs(at - 25.0 * i), 0.0) for i in range(near)]
        outer = mask_ref[0, t]
        inner = mask_ref[1, t]
        values = []
        for nc in range(6):
            total = None
            for i in range(near):
                term = weights[i] * north[t, nc * c_east + first + i]
                total = term if total is None else total + term
            values.append(total)
            parts[nc, x] = outer * total
            parts[6 + nc, x] = inner * total
            if t == 1:
                inc_held[pl.ds(nc * lev * rows + cell, lev, stride=rows), :] = total[:, :LANE]
        for n in range(2):
            for q, mask in enumerate((outer, inner)):
                moved = east_flow([mask * values[3 * n + c] for c in range(3)], coef, x)
                for i in range(3):
                    flow[6 * n + 3 * q + i, x] = moved[i]

    rows_loop(0, rows, rows, lambda cell: east(cell + 2, 1, cell))
    for r in range(2):
        east(r, 0, rows - 2 + r)
        east(rows + 2 + r, 2, r)
    sends = [pltpu.make_async_copy(a, b, sems.at[i]) for i, (a, b) in enumerate(outs)]
    sends[0].start()

    def forcing(step, x, t, width):
        outside = apply_row(
            lambda c, r: parts[3 * step + c, r], lambda i, r: flow[6 * step + i, r], coef, x, width
        )
        inside = apply_row(
            lambda c, r: parts[6 + 3 * step + c, r], lambda i, r: flow[6 * step + 3 + i, r], coef, x, width
        )
        outer = mask_ref[0, t][:, :width]
        inner = mask_ref[1, t][:, :width]
        return [inner * outside[c] - outer * inside[c] for c in range(3)]

    def middle(x, t):
        force = forcing(0, x, t, WIDE)
        for c in range(3):
            value = base_ref[c, x] + scale_ref[x] * force[c]
            mid[c, x] = value
            if t == 1:
                mid_held[pl.ds(c * lev * rows + x - 2, lev, stride=rows), :] = value[:, :LANE]

    middle(1, 0)
    rows_loop(2, rows + 2, rows // 2, lambda x: middle(x, 1))
    middle(rows + 2, 2)
    sends[1].start()

    def flows(x):
        moved = east_flow([mid[c, x] for c in range(3)], coef, x)
        for i in range(3):
            flow[12 + i, x] = moved[i]

    rows_loop(1, rows + 3, rows + 2, flows)

    def last(x):
        force = forcing(1, x, 1, LANE)
        applied = apply_row(lambda c, r: mid[c, r], lambda i, r: flow[12 + i, r], coef, x, LANE)
        scale = scale_ref[x, :, :LANE]
        for c in range(3):
            now = now_ref[pl.ds(c * lev * rows + x - 2, lev, stride=rows), :]
            current = mid[c, x, :, :LANE]
            next_held[pl.ds(c * lev * rows + x - 2, lev, stride=rows), :] = (
                2.0 * current - now + scale * (applied[c] + force[c])
            )

    rows_loop(2, rows + 2, rows, last)
    sends[2].start()
    for send in sends:
        send.wait()


def specs(text):
    space = {"v": VMEM, "s": SMEM, "h": pltpu.HBM}
    return [pl.BlockSpec(memory_space=space[kind]) for kind in text]


def f32(*shape):
    return jax.ShapeDtypeStruct(shape, jnp.float32)


def neighbours(axis, step):
    count = lax.axis_size(axis)
    return [(i, i + step) for i in range(count) if 0 <= i + step < count]


def local(disp_now, disp_prev, density, moduli, coarse, block_route, ranges, offsets):
    _, lev, rows, north_cells = disp_now.shape
    groups = lev // 2
    c_east = (rows + 23) * 4 // 25 + 2
    c_north = (north_cells + 23) * 4 // 25 + 2
    block_hold = coarse.shape[0]
    samples = coarse.shape[1] // 6
    n_x = lax.axis_size("gx")
    n_y = lax.axis_size("gy")
    assert lev == 8 and north_cells == LANE and block_hold == 2
    assert (c_east, c_north) == (8, 26) and 6 * (rows + 4) <= LANE
    now, prev, dens, mods = (a.reshape(-1, north_cells) for a in (disp_now, disp_prev, density, moduli))
    wide = rows + 4
    shifts = offsets.transpose(0, 3, 1, 2)
    limit = pltpu.CompilerParams(vmem_limit_bytes=16 * 2**20)
    assert n_x % 2 == 0

    payload, first, last = pl.pallas_call(
        functools.partial(pre_kernel, lev, rows, groups, samples),
        out_shape=(f32(40, LANE), f32(15, lev, LANE), f32(15, lev, LANE)),
        in_specs=specs("hhhhhss"),
        out_specs=specs("vvv"),
        scratch_shapes=[VMEM((24, WIDE), jnp.float32)]
        + [VMEM(a.shape, jnp.float32) for a in (coarse, now, prev, dens, mods)]
        + [pltpu.SemaphoreType.DMA((5,))],
        compiler_params=limit,
        name="pre",
    )(*(pltpu.with_memory_space_constraint(a, pltpu.HBM) for a in (coarse, now, prev, dens, mods, shifts, ranges)))
    half = n_x * n_y // 2
    twin = lax.ppermute(payload, "gx", [(i, (i + n_x // 2) % n_x) for i in range(n_x)])
    before = lax.ppermute(last, "gx", neighbours("gx", 1))
    after = lax.ppermute(first, "gx", neighbours("gx", -1))
    chunk = jnp.concatenate([payload, twin], axis=0)
    got = lax.all_to_all(
        jnp.broadcast_to(chunk[None], (half,) + chunk.shape),
        ("gx", "gy"),
        split_axis=0,
        concat_axis=0,
        tiled=True,
        axis_index_groups=[list(range(half)), list(range(half, 2 * half))],
    ).reshape(2 * half, 40, LANE)
    to_west, to_east, meta = pl.pallas_call(
        functools.partial(pack_kernel, lev, rows),
        out_shape=(f32(4, lev, LANE), f32(4, lev, LANE), f32(lev, LANE)),
        in_specs=specs("vvvvvvv"),
        out_specs=specs("vvv"),
        cost_estimate=pl.CostEstimate(flops=2000000, bytes_accessed=1000000, transcendentals=0),
        compiler_params=limit,
        name="pack",
    )(now, prev, dens, mods, before, after, first)
    west = lax.ppermute(to_east, "gy", neighbours("gy", 1))
    east = lax.ppermute(to_west, "gy", neighbours("gy", -1))
    place = jnp.stack([lax.axis_index("gx"), lax.axis_index("gy")]).astype(jnp.int32)
    index = pl.pallas_call(
        functools.partial(index_kernel, groups, n_x, n_y),
        out_shape=jax.ShapeDtypeStruct((9 * groups + 1,), jnp.int32),
        in_specs=specs("ss"),
        out_specs=specs("s")[0],
        compiler_params=limit,
        cost_estimate=pl.CostEstimate(flops=2000000, bytes_accessed=1000, transcendentals=0),
        name="index",
    )(block_route, place)
    prepared = pl.pallas_call(
        functools.partial(prep_kernel, lev, rows, groups, c_north),
        out_shape=(
            f32(2, wide, lev, WIDE),
            f32(3, wide, lev, WIDE),
            f32(wide, lev, WIDE),
            f32(2, 3, lev, WIDE),
            f32(3, 3, 2, lev, LANE),
            f32(3, lev, WIDE),
            jax.ShapeDtypeStruct((3, LANE, LANE), jnp.bfloat16),
            jax.ShapeDtypeStruct((3, WIDE, LANE), jnp.bfloat16),
        ),
        in_specs=specs("v" * 9),
        out_specs=specs("v" * 8),
        scratch_shapes=[
            VMEM((3, wide, lev, WIDE), jnp.float32),
            VMEM((3, wide, lev, WIDE), jnp.float32),
            VMEM((COEFS, wide, lev, WIDE), jnp.float32),
        ],
        cost_estimate=pl.CostEstimate(flops=10000000, bytes_accessed=3000000, transcendentals=0),
        compiler_params=limit,
        name="prep",
    )(now, prev, dens, mods, before, after, west, east, meta)
    mods_x, base, scale, mask, level_w, shift, own_hat, side_hat = prepared
    incident, mid, nxt = pl.pallas_call(
        functools.partial(finish_kernel, lev, rows, groups, c_east, c_north),
        out_shape=(
            f32(6 * lev * rows, LANE),
            f32(3 * lev * rows, LANE),
            f32(3 * lev * rows, LANE),
        ),
        in_specs=specs("vsvvvvvvvvv"),
        out_specs=specs("hhh"),
        scratch_shapes=[
            VMEM((3, 3, c_east, 16, LANE), jnp.float32),
            VMEM((3, 6 * c_east * lev, LANE), jnp.float32),
            VMEM((3, 6 * c_east * lev, WIDE), jnp.float32),
            VMEM((3, 6 * c_east, lev, WIDE), jnp.float32),
            VMEM((12, wide, lev, WIDE), jnp.float32),
            VMEM((15, wide, lev, WIDE), jnp.float32),
            VMEM((3, wide, lev, WIDE), jnp.float32),
            VMEM((COEFS, wide, lev, WIDE), jnp.float32),
            VMEM((6 * lev * rows, LANE), jnp.float32),
            VMEM((3 * lev * rows, LANE), jnp.float32),
            VMEM((3 * lev * rows, LANE), jnp.float32),
            pltpu.SemaphoreType.DMA((3,)),
        ],
        cost_estimate=pl.CostEstimate(flops=20000000, bytes_accessed=6000000, transcendentals=0),
        compiler_params=limit,
        name="finish",
    )(got, index, mods_x, base, scale, mask, level_w, shift, own_hat, side_hat, now)
    return (
        incident.reshape(2, 3, lev, rows, north_cells),
        mid.reshape(disp_now.shape),
        nxt.reshape(disp_now.shape),
    )


def solution(mesh):
    return jax.shard_map(
        local,
        mesh=mesh,
        in_specs=(
            P(None, None, "gx", "gy"),
            P(None, None, "gx", "gy"),
            P(None, "gx", "gy"),
            P(None, None, "gx", "gy"),
            P(("gx", "gy"), None, None),
            P(),
            P("gx", "gy", None),
            P("gx", "gy", None, None),
        ),
        out_specs=(
            P(None, None, None, "gx", "gy"),
            P(None, None, "gx", "gy"),
            P(None, None, "gx", "gy"),
        ),
        check_vma=False,
    )
```
